32 devices in a mesh: seq: 8 (over z, core), head: 4 (over y, x).
Axes of the slice: x: 2, y: 2, z: 4, core: 2. Of those that a mesh axis runs over, the one named last changes fastest.
Arguments:
- grad_output: bfloat16 [8192, 4096], P('seq', 'head'), may hold values from -6 to 6
- out_weight: bfloat16 [4096, 8192], P('seq', 'head'), may hold values from -0.0625 to 0.0625
- ssd_out: bfloat16 [8192, 8192], P('seq', 'head'), may hold values from -520 to 520
- gate: bfloat16 [8192, 8192], P('seq', 'head'), may hold values from -5 to 5
- norm_weight: float32 [8192], P('head'), may hold values from 0.5 to 1.5
- time_step: float32 [128, 8192], P('head', 'seq'), may hold values from 0.01 to 0.1
- log_decay: float32 [128, 8192], P('head', 'seq'), may hold values from -0.7 to 0
- state_in: bfloat16 [8192, 8, 128], P('seq'), may hold values from -1.796875 to 1.796875
- state_out: bfloat16 [8192, 8, 128], P('seq'), may hold values from -1.796875 to 1.796875
- skip: float32 [128], P('head'), may hold values from 0.5 to 1.5
Outputs:
- grad_x: bfloat16 [8192, 8192], P('seq', 'head')
- grad_gate: bfloat16 [8192, 8192], P('seq', 'head')
- grad_out_weight: float32 [4096, 8192], P('seq', 'head')
The draws below stay inside these ranges and needn't reach their ends.
All inputs are finite; a program needn't handle non-finite values.
Results may differ from the reference program's by a relative error of at most 0.014.
Values may be sent and summed in bfloat16 or wider, within the bound.
A program may use at most 192 MiB of HBM per device.

```python
import math
from functools import partial
import jax
import jax.numpy as jnp
from jax import lax

D = 4096
HEADS = 128
HDIM = 64
NSTATE = 128
GROUPS = 8
BLOCK_LEN = 256
TOK_DEV = 1024
TOKENS = 8192
DI = 8192


def draw_log_decay(key, part):
    keys = jax.random.split(jax.random.fold_in(key, 11), 7)
    order = jax.random.permutation(keys[0], HEADS)
    slow_count = HEADS // 2
    slow_heads = order < slow_count
    chain = float(TOKENS)
    slow_rate = jnp.exp(jax.random.uniform(keys[1], (HEADS,), jnp.float32, math.log(0.1 / chain), math.log(0.5 / chain)))
    fast_rate = jnp.exp(jax.random.uniform(keys[2], (HEADS,), jnp.float32, math.log(2.0 / chain), math.log(0.035)))
    fading_speed = jnp.where(slow_heads, slow_rate, fast_rate)
    blocks = TOKENS // TOK_DEV
    multiplier_coefficient = jnp.exp2(jax.random.uniform(keys[3], (HEADS, blocks), jnp.float32, -1.0, 1.0))
    multiplier_coefficient = jnp.repeat(multiplier_coefficient, TOK_DEV, axis=1)
    approximate_guess = jax.random.uniform(keys[4], (HEADS, TOKENS), jnp.float32, 0.5, 1.5)
    seat_locations = jax.random.randint(keys[5], (3,), 0, TOKENS)
    increment_lengths = jax.random.uniform(keys[6], (3,), jnp.float32, 0.22, 0.51)
    sequence_indices = jnp.arange(TOKENS)
    clustered_spans = jnp.max(jnp.where(sequence_indices[None, :] == seat_locations[:, None], increment_lengths[:, None], 0.0), axis=0)
    return (-(fading_speed[:, None] * multiplier_coefficient * approximate_guess) - clustered_spans[None, :]).astype(jnp.float32)


def draw_ssd_out(key, part):
    keys = jax.random.split(jax.random.fold_in(key, 23), 4)
    row_scale = jnp.exp(jax.random.uniform(keys[0], (TOKENS,), jnp.float32, 0.0, math.log(10.0)))
    column_scale = jnp.exp(jax.random.uniform(keys[1], (DI,), jnp.float32, math.log(0.3), math.log(3.0)))
    ramp = jnp.arange(DI, dtype=jnp.float32) / DI
    base = jax.random.truncated_normal(keys[3], -4.0, 4.0, (TOKENS, DI), jnp.float32)
    rising = jnp.power(3.0, 0.5 * ramp)
    return (base * row_scale[:, None] * (column_scale * rising)[None, :]).astype(jnp.bfloat16)


def spiked(entries, key, source, target, parts, factor):
    def block_of(dim):
        return (jnp.arange(entries.shape[dim]) // (entries.shape[dim] // parts)).reshape((-1,) + (1,) * (entries.ndim - 1 - dim))

    one_side = jax.random.permutation(key, parts)[block_of(target)]
    other_side = (block_of(target) + parts // 2) % parts
    return jnp.where((block_of(source) == one_side) | (block_of(source) == other_side), factor * entries, entries)


def block_scale(own_key, extent, pieces, low, high):
    def one(dim, blocks):
        steps = jax.random.uniform(jax.random.fold_in(jax.random.fold_in(own_key, 6), dim), (blocks,), jnp.float32, low / len(pieces), high / len(pieces))
        return jnp.repeat(jnp.exp(steps), extent[dim] // blocks).reshape((-1,) + (1,) * (len(extent) - dim - 1))

    level = one(*pieces[0])
    for cut in pieces[1:]:
        level = level * one(*cut)
    return level


def gaussian(own_key, shape, scale, most, shards=(), held_as=jnp.bfloat16):
    loudness = block_scale(own_key, shape, shards, -0.22, 0.18) if shards else 1.0
    drawn = jax.random.normal(own_key, shape, jnp.float32) * scale * loudness
    return jnp.minimum(jnp.maximum(drawn, -most), most).astype(held_as)


def heavy_noise(stream_key, extent, width, bound, cuts, heavy, kind=jnp.bfloat16):
    drawn = width * jax.random.normal(stream_key, extent, jnp.float32)
    if cuts:
        drawn = drawn * block_scale(stream_key, extent, cuts, -0.22, 0.18)
    return jnp.clip(spiked(drawn, jax.random.fold_in(stream_key, 3), *heavy), -bound, bound).astype(kind)


def setup_inputs(seed: int = 0) -> dict:
    seeds = jax.random.split(jax.random.key(seed), 11)
    return {
        "grad_output": heavy_noise(seeds[0], (TOKENS, D), 1.0, 6.0, ((0, 8), (1, 4)), (0, 1, 8, 2.0)),
        "out_weight": gaussian(seeds[1], (D, DI), DI ** -0.5, 0.0625, ((0, 8), (1, 4))),
        "ssd_out": draw_ssd_out(jax.random.fold_in(seeds[10], 71), 0),
        "gate": gaussian(seeds[3], (TOKENS, DI), 1.0, 5.0, ((0, 8), (1, 4))),
        "norm_weight": jnp.clip(1.0 + 0.1 * jax.random.normal(seeds[4], (DI,), jnp.float32), 0.5, 1.5),
        "time_step": jnp.clip(jnp.exp(math.log(0.1) - 2.3025851 * jax.random.uniform(seeds[5], (HEADS, TOKENS), jnp.float32) ** block_scale(seeds[5], (HEADS, TOKENS), ((0, 4), (1, 8)), -0.2, 0.2)), 0.01, 0.1),
        "log_decay": draw_log_decay(jax.random.fold_in(seeds[10], 71), 0),
        "state_in": gaussian(seeds[7], (TOKENS, GROUPS, NSTATE), 0.3, 1.796875, ((0, 8),)),
        "state_out": gaussian(seeds[8], (TOKENS, GROUPS, NSTATE), 0.3, 1.796875, ((0, 8),)),
        "skip": jnp.clip(0.5 + 1.0 * jax.random.uniform(seeds[9], (HEADS,), jnp.float32) ** block_scale(seeds[9], (HEADS,), ((0, 4),), -0.2, 0.2), 0.5, 1.5),
    }


epsilon = 1e-05

def head_grad(head, grad_ssd, time_step, log_decay, state_in, state_out, skip):
    group = (head // (HEADS // GROUPS)).astype(jnp.int32)
    blocks = TOKENS // BLOCK_LEN
    start_col = (head * HDIM).astype(jnp.int32)
    grad_cols = lax.dynamic_slice_in_dim(grad_ssd, start_col, HDIM, 1).astype(jnp.float32)
    grad_cols = grad_cols.reshape(blocks, BLOCK_LEN, HDIM)
    b_rows = lax.dynamic_index_in_dim(state_in, group, 1, keepdims=False).astype(jnp.float32)
    b_rows = b_rows.reshape(blocks, BLOCK_LEN, NSTATE)
    c_rows = lax.dynamic_index_in_dim(state_out, group, 1, keepdims=False).astype(jnp.float32)
    c_rows = c_rows.reshape(blocks, BLOCK_LEN, NSTATE)
    rates = lax.dynamic_index_in_dim(log_decay, head, 0, keepdims=False).reshape(blocks, BLOCK_LEN)
    step_sizes = lax.dynamic_index_in_dim(time_step, head, 0, keepdims=False).reshape(blocks, BLOCK_LEN)
    skip_head = lax.dynamic_index_in_dim(skip, head, 0, keepdims=False)
    cumulative = jnp.cumsum(rates, axis=1)
    block_total = cumulative[:, -1]
    sequence_indices = jnp.arange(BLOCK_LEN)
    upper_mask = sequence_indices[None, :] >= sequence_indices[:, None]
    scores = jnp.einsum('ktn,ksn->kts', b_rows, c_rows)
    log_gap = cumulative[:, None, :] - cumulative[:, :, None]
    block_weights = jnp.where(upper_mask, scores * jnp.exp(jnp.minimum(log_gap, 0.0)), 0.0).astype(jnp.bfloat16)
    block_weights = lax.optimization_barrier(block_weights).astype(jnp.float32)
    within = jnp.einsum('kts,ksp->ktp', block_weights, grad_cols)
    scaled = (jnp.exp(cumulative)[:, :, None] * grad_cols).astype(jnp.bfloat16)
    scaled = lax.optimization_barrier(scaled).astype(jnp.float32)
    block_state = jnp.einsum('ksp,ksn->kpn', scaled, c_rows)

    def fold_block(carried, inputs):
        state_now, total_now = inputs
        return (state_now + jnp.exp(total_now) * carried, carried)
    unused, carry = lax.scan(fold_block, jnp.zeros((HDIM, NSTATE), jnp.float32), (block_state, block_total), reverse=True)
    carry_low = lax.optimization_barrier(carry.astype(jnp.bfloat16)).astype(jnp.float32)
    across = jnp.einsum('kpn,ktn->ktp', carry_low, b_rows) * jnp.exp(block_total[:, None] - cumulative)[:, :, None]
    result = step_sizes[:, :, None] * (within + across) + skip_head * grad_cols
    return result.reshape(TOKENS, HDIM).astype(jnp.bfloat16)

def reference(grad_output, out_weight, ssd_out, gate, norm_weight, time_step, log_decay, state_in, state_out, skip):
    values = ssd_out.astype(jnp.float32)
    gate_values = gate.astype(jnp.float32)
    sigmoid_gate = jax.nn.sigmoid(gate_values)
    silu_gate = gate_values * sigmoid_gate
    gated_values = values * silu_gate
    inverse_rms = lax.rsqrt(lax.optimization_barrier(jnp.mean(gated_values * gated_values, axis=1, keepdims=True)) + epsilon)
    normed = (gated_values * inverse_rms * norm_weight).astype(jnp.bfloat16)
    normed_grad = jnp.dot(grad_output, out_weight, preferred_element_type=jnp.float32)
    weighted = lax.optimization_barrier(jnp.sum(norm_weight * normed_grad * gated_values, axis=1, keepdims=True))
    gated_grad = inverse_rms * norm_weight * normed_grad - gated_values * inverse_rms ** 3 * weighted / DI
    grad_gate = (gated_grad * values * sigmoid_gate * (1.0 + gate_values * (1.0 - sigmoid_gate))).astype(jnp.bfloat16)
    grad_ssd = (gated_grad * silu_gate).astype(jnp.bfloat16)
    grad_out_weight = jnp.dot(grad_output.T, normed, preferred_element_type=jnp.float32) * (1.0 / math.sqrt(TOKENS))
    per_head = lax.map(partial(head_grad, grad_ssd=grad_ssd, time_step=time_step, log_decay=log_decay, state_in=state_in, state_out=state_out, skip=skip), jnp.arange(HEADS, dtype=jnp.int32))
    grad_x = jnp.transpose(per_head, (1, 0, 2)).reshape(TOKENS, DI)
    return (grad_x, grad_gate, grad_out_weight)
```

```python
import functools
import math

import jax
import jax.numpy as jnp
from jax import lax
from jax.experimental import pallas as pl
from jax.experimental.pallas import tpu as pltpu
from jax.sharding import PartitionSpec as P

HEADS = 128
GROUPS = 8
BLOCK_LEN = 256
MESH = pl.DeviceIdType.MESH
F32 = jnp.float32
BF16 = jnp.bfloat16
ROWS = 16
TILE_ROWS = 64


epsilon = 1e-05


def remote(src, dst, send_sem, recv_sem, **device):
    return pltpu.make_async_remote_copy(
        src_ref=src,
        dst_ref=dst,
        send_sem=send_sem,
        recv_sem=recv_sem,
        device_id=device,
        device_id_type=MESH,
    )


def lane_sum(x):
    total = x[:, 0:128]
    for j in range(1, x.shape[1] // 128):
        total = total + x[:, j * 128 : (j + 1) * 128]
    return total


def mixer_kernel(
    dims,
    g_ref,
    w_ref,
    y_ref,
    z_ref,
    nw_ref,
    gate_out,
    grad_out,
    gow_out,
    wfull,
    gfull,
    nbuf,
    acc,
    pair,
    chain,
    pst,
    ownp,
    gt,
    wbuf,
    ybuf,
    zbuf,
    obuf,
    sqp,
    sqx,
    wgx,
    invc,
    cfc,
    ag_recv,
    ag_r,
    ag_l,
    ag_p,
    g_recv,
    g_send,
    sq_recv,
    sq_send,
    wg_recv,
    wg_send,
    pair_recv,
    pair_send,
    ch_recv,
    ch_send,
    loc,
    wsem,
    in_sem,
    out_sem,
):
    S, H, T, F, Wr, C = dims
    Z = S // 2
    half = Wr // 2
    nsub = F // Wr
    DI = C * H
    TN = min(256, C)
    s = lax.axis_index("seq")
    h = lax.axis_index("head")
    z = s // 2
    c = s % 2
    zm = Z - 1 - z
    partner = s + 1 - 2 * c
    others = range(1, H)

    barrier = pltpu.get_barrier_semaphore()
    pl.semaphore_signal(barrier, inc=1, device_id={"seq": partner}, device_id_type=MESH)
    for j in others:
        pl.semaphore_signal(barrier, inc=1, device_id={"head": h ^ j}, device_id_type=MESH)

    @pl.when(z > 0)
    def _():
        pl.semaphore_signal(barrier, inc=1, device_id={"seq": s - 2}, device_id_type=MESH)

    @pl.when(z < Z - 1)
    def _():
        pl.semaphore_signal(barrier, inc=1, device_id={"seq": s + 2}, device_id_type=MESH)

    peers = H + jnp.where(z > 0, 1, 0) + jnp.where(z < Z - 1, 1, 0)
    pl.semaphore_wait(barrier, peers)

    def w_src(k, ch, own):
        return w_ref.at[pl.ds(ch * half, half)] if own else wfull.at[2 * k + c, ch]

    def w_right(k, ch, own=False):
        q = 2 * k + c
        return remote(
            w_src(k, ch, own), wfull.at[q, ch], ag_r.at[k, ch], ag_recv.at[q, ch], seq=s + 2
        )

    def w_left(k, ch, own=False):
        q = 2 * k + c
        return remote(
            w_src(k, ch, own), wfull.at[q, ch], ag_l.at[k, ch], ag_recv.at[q, ch], seq=s - 2
        )

    def w_swap(k, ch, own=False):
        q = 2 * k + c
        return remote(
            w_src(k, ch, own), wfull.at[q, ch], ag_p.at[k, ch], ag_recv.at[q, ch], seq=partner
        )

    def w_arrived(q, ch):
        remote(
            wfull.at[q, ch], wfull.at[q, ch], ag_p.at[0, 0], ag_recv.at[q, ch], seq=partner
        ).wait_recv()

    for ch in range(2):

        @pl.when(z < Z - 1)
        def _():
            w_right(z, ch, True).start()

        @pl.when(z > 0)
        def _():
            w_left(z, ch, True).start()

        w_swap(z, ch, True).start()

    def g_own(sub, hf):
        return g_ref.at[:, pl.ds(sub * Wr + hf * half, half)]

    def g_local(sub, hf):
        return pltpu.make_async_copy(
            g_own(sub, hf), gfull.at[h * nsub + sub, hf], loc.at[sub, hf]
        )

    for sub in range(nsub):
        for hf in range(2):
            g_local(sub, hf).start()

    tiles = T // TILE_ROWS

    def fetch(t, slot):
        rows = pl.ds(t * TILE_ROWS, TILE_ROWS)
        return (
            pltpu.make_async_copy(y_ref.at[rows], ybuf.at[slot], in_sem.at[0, slot]),
            pltpu.make_async_copy(z_ref.at[rows], zbuf.at[slot], in_sem.at[1, slot]),
        )

    def stream(body):
        for copy in fetch(0, 0):
            copy.start()

        @pl.loop(0, tiles)
        def _(t):
            slot = t % 2

            @pl.when(t + 1 < tiles)
            def _():
                for copy in fetch(t + 1, 1 - slot):
                    copy.start()

            for copy in fetch(t, slot):
                copy.wait()
            body(t, slot)

    def square_tile(t, slot):
        @pl.loop(0, TILE_ROWS // ROWS)
        def _(r):
            rows = pl.ds(r * ROWS, ROWS)
            at = pl.ds(t * TILE_ROWS + r * ROWS, ROWS)
            gv = zbuf[slot, rows, :].astype(F32)
            gated = ybuf[slot, rows, :].astype(F32) * (gv * jax.nn.sigmoid(gv))
            acc[at, :] = gated
            sqp[at, :] = lane_sum(gated * gated)

    stream(square_tile)

    def share(buf, send, recv):
        buf[h] = jnp.broadcast_to(jnp.sum(sqp[...].T, axis=0, keepdims=True), (8, T))
        for j in others:
            remote(buf.at[h], buf.at[h], send.at[j], recv.at[h], head=h ^ j).start()

    def shared(buf, send, recv):
        for j in others:
            remote(buf.at[h ^ j], buf.at[h ^ j], send.at[j], recv.at[h ^ j], head=h ^ j).wait_recv()
        total = buf[0, 0:1, :]
        for j in others:
            total = total + buf[j, 0:1, :]
        for j in others:
            remote(buf.at[h], buf.at[h], send.at[j], recv.at[h], head=h ^ j).wait_send()
        return total

    share(sqx, sq_send, sq_recv)

    def g_to(j, sub, hf):
        q = h * nsub + sub
        return remote(
            g_own(sub, hf), gfull.at[q, hf], g_send.at[j, sub, hf], g_recv.at[q, hf], head=h ^ j
        )

    def g_relay(j, frm, sub, hf):
        q = (h ^ frm) * nsub + sub
        return remote(
            gfull.at[q, hf], gfull.at[q, hf], g_send.at[3, sub, hf], g_recv.at[q, hf], head=h ^ j
        )

    def g_arrived(j, sub, hf):
        q = (h ^ j) * nsub + sub
        remote(
            gfull.at[q, hf], gfull.at[q, hf], g_send.at[j, sub, hf], g_recv.at[q, hf], head=h ^ j
        ).wait_recv()

    subs = range(nsub)
    if H == 4:
        for sub in subs:
            g_to(1, sub, 0).start()
            g_to(2, sub, 1).start()
    else:
        for j in others:
            for sub in subs:
                for hf in range(2):
                    g_to(j, sub, hf).start()

    inv_row = lax.rsqrt(shared(sqx, sq_send, sq_recv) / DI + epsilon)
    invc[...] = jnp.broadcast_to(inv_row, (128, T)).T

    @pl.loop(0, T // ROWS)
    def _(r):
        at = pl.ds(r * ROWS, ROWS)
        nbuf[at, :] = (acc[at, :] * invc[at, 0:1] * nw_ref[...]).astype(BF16)

    for sub in subs:
        for hf in range(2):
            g_local(sub, hf).wait()
    if H == 4:
        for sub in subs:
            g_arrived(1, sub, 0)
            g_relay(2, 1, sub, 0).start()
        for sub in subs:
            g_arrived(2, sub, 1)
            g_relay(1, 2, sub, 1).start()
        for sub in subs:
            g_to(1, sub, 1).start()
            g_to(2, sub, 0).start()

    def pair_copy(k, cx, d, ch):
        return remote(
            pst.at[d, ch], pair.at[k, cx], pair_send.at[d, ch], pair_recv.at[k, cx], seq=partner
        )

    def rs_prep(k, cx, d, ch, slot):
        gt[0:half, :] = gfull[2 * k + 1 - c, cx].T
        gt[half:Wr, :] = gfull[2 * k + c, cx].T

        @pl.loop(0, C // TN)
        def _(t):
            cols = pl.ds(pl.multiple_of(t * TN, TN), TN)
            part = jnp.dot(gt[...], nbuf[:, cols], preferred_element_type=F32)
            pst[d, ch, :, cols] = part[:half].astype(BF16)
            ownp[slot, :, cols] = part[half:]

        pair_copy(k, cx, d, ch).start()

    def chain_right(k, cx):
        return remote(
            chain.at[k, cx], chain.at[k, cx], ch_send.at[k, cx], ch_recv.at[k, cx], seq=s + 2
        )

    def chain_left(k, cx):
        to = jnp.where(k == z - 1, Z, k)
        return remote(
            chain.at[k, cx], chain.at[to, cx], ch_send.at[k, cx], ch_recv.at[to, cx], seq=s - 2
        )

    def chain_arrived(k, cx):
        remote(
            chain.at[k, cx], chain.at[k, cx], ch_send.at[0, 0], ch_recv.at[k, cx], seq=partner
        ).wait_recv()

    def rs_sum(k, cx, d, ch, chained):
        pair_copy(k, cx, d, ch).wait_recv()

        @pl.when(chained)
        def _():
            chain_arrived(k, cx)

            @pl.loop(0, half // ROWS)
            def _(r):
                at = pl.ds(r * ROWS, ROWS)
                chain[k, cx, at, :] = (
                    ownp[d, at, :] + pair[k, cx, at, :].astype(F32) + chain[k, cx, at, :].astype(F32)
                ).astype(BF16)

        @pl.when(jnp.logical_not(chained))
        def _():
            @pl.loop(0, half // ROWS)
            def _(r):
                at = pl.ds(r * ROWS, ROWS)
                chain[k, cx, at, :] = (ownp[d, at, :] + pair[k, cx, at, :].astype(F32)).astype(BF16)

    def half_of(k, ch):
        if H != 4:
            return ch
        return jnp.where((2 * k * Wr // F) ^ h == 2, 1 - ch, ch)

    near = jnp.minimum(z, zm)

    def plane_of(p):
        d = (p + 1) // 2
        close = jnp.where(p % 2 == 1, z - d, z + d)
        far = jnp.where(z < zm, z + (p - near), z - (p - near))
        return jnp.where(p <= 2 * near, close, far)

    def w_load(src, par, ch):
        return pltpu.make_async_copy(src, wbuf.at[par, ch], wsem.at[par, ch])

    def project(p, first):
        k = plane_of(p)
        for ch in range(2):
            w_arrived(2 * k + 1 - c, ch)
        for par in range(2):
            for ch in range(2):
                mine = jnp.logical_and(k == z, c == par)

                @pl.when(mine)
                def _():
                    w_load(w_ref.at[pl.ds(ch * half, half)], par, ch).start()

                @pl.when(jnp.logical_not(mine))
                def _():
                    w_load(wfull.at[2 * k + par, ch], par, ch).start()

        for par in range(2):
            for ch in range(2):
                w_load(wfull.at[2 * k + par, ch], par, ch).wait()

        @pl.loop(0, C // TN)
        def _(t):
            cols = pl.ds(pl.multiple_of(t * TN, TN), TN)
            total = None if first else acc[:, cols]
            for par in range(2):
                for ch in range(2):
                    part = jnp.dot(
                        gfull[2 * k + par, ch], wbuf[par, ch, :, cols], preferred_element_type=F32
                    )
                    total = part if total is None else total + part
            acc[:, cols] = total

    @pl.loop(2, 2 * Z)
    def _(i):
        slot = i // 2
        ch = i % 2

        @pl.when(z - slot >= 0)
        def _():
            k = z - slot
            w_arrived(2 * k + c, ch)

            @pl.when(z < Z - 1)
            def _():
                w_right(k, ch).start()

            w_swap(k, ch).start()

        @pl.when(z + slot <= Z - 1)
        def _():
            k = z + slot
            w_arrived(2 * k + c, ch)

            @pl.when(z > 0)
            def _():
                w_left(k, ch).start()

            w_swap(k, ch).start()

        @pl.when(i == 2)
        def _():
            for j in (others if H != 4 else (3,)):
                for sub in subs:
                    for hf in range(2):
                        g_arrived(j, sub, hf)

        if H == 4:

            @pl.when(i == 3)
            def _():
                for sub in subs:
                    g_arrived(1, sub, 1)
                    g_arrived(2, sub, 0)

        go_right = jnp.logical_and(slot > z, z < Z - 1)
        go_left = jnp.logical_and(slot > zm, z > 0)
        kr = Z + z - slot
        kl = slot - Z + z

        @pl.when(go_right)
        def _():
            @pl.when(slot - 1 > z)
            def _():
                pair_copy(kr, 0, 0, ch).wait_send()

            rs_prep(kr, half_of(kr, ch), 0, ch, 0)

        @pl.when(go_left)
        def _():
            @pl.when(slot - 1 > zm)
            def _():
                pair_copy(kl, 0, 1, ch).wait_send()

            rs_prep(kl, half_of(kl, ch), 1, ch, 1)

        @pl.when(go_right)
        def _():
            cx = half_of(kr, ch)
            rs_sum(kr, cx, 0, ch, z > 0)
            chain_right(kr, cx).start()

        @pl.when(go_left)
        def _():
            cx = half_of(kl, ch)
            rs_sum(kl, cx, 1, ch, z < Z - 1)
            chain_left(kl, cx).start()

        @pl.when(i == 4)
        def _():
            project(0, True)

        lo = jnp.where(i == 4, 1, jnp.where(i == 5, 2, slot))
        hi = jnp.where(
            i == 4, 2, jnp.where(i == 5, 3, jnp.where((slot >= 3) & (ch == 1), slot + 1, slot))
        )
        hi = jnp.where(i < 4, lo, jnp.minimum(hi, Z - 1))

        @pl.loop(lo, hi)
        def _(p):
            project(p, False)

    project(Z - 1, False)

    @pl.loop(0, T // ROWS)
    def _(r):
        at = pl.ds(r * ROWS, ROWS)
        sqp[at, :] = lane_sum(acc[at, :] * nbuf[at, :].astype(F32))

    share(wgx, wg_send, wg_recv)
    weighted = shared(wgx, wg_send, wg_recv) / DI
    cfc[...] = jnp.broadcast_to(weighted, (128, T)).T * invc[...] * invc[...]

    def put(t, slot):
        rows = pl.ds(t * TILE_ROWS, TILE_ROWS)
        return (
            pltpu.make_async_copy(obuf.at[0, slot], gate_out.at[rows], out_sem.at[0, slot]),
            pltpu.make_async_copy(obuf.at[1, slot], grad_out.at[rows], out_sem.at[1, slot]),
        )

    def grad_tile(t, slot):
        @pl.when(t >= 2)
        def _():
            for copy in put(t - 2, slot):
                copy.wait()

        @pl.loop(0, TILE_ROWS // ROWS)
        def _(r):
            rows = pl.ds(r * ROWS, ROWS)
            at = pl.ds(t * TILE_ROWS + r * ROWS, ROWS)
            gv = zbuf[slot, rows, :].astype(F32)
            values = ybuf[slot, rows, :].astype(F32)
            sig = jax.nn.sigmoid(gv)
            silu = gv * sig
            gg = invc[at, 0:1] * nw_ref[...] * acc[at, :] - values * silu * cfc[at, 0:1]
            obuf[0, slot, rows, :] = (gg * values * sig * (1.0 + gv * (1.0 - sig))).astype(BF16)
            obuf[1, slot, rows, :] = (gg * silu).astype(BF16)

        for copy in put(t, slot):
            copy.start()

    stream(grad_tile)
    for t in (tiles - 2, tiles - 1):
        for copy in put(t, t % 2):
            copy.wait()

    for ch in range(2):

        @pl.when(Z - 1 > z)
        def _():
            pair_copy(z, ch, 0, ch).wait_send()

        rs_prep(z, ch, 0, ch, ch)

    scale = 1.0 / math.sqrt(T * S)

    def gow_copy(ch):
        rows = pl.ds(ch * half, half)
        return pltpu.make_async_copy(acc.at[rows], gow_out.at[rows], out_sem.at[0, ch])

    for ch in range(2):
        pair_copy(z, ch, 0, ch).wait_recv()

        @pl.loop(0, half // ROWS)
        def _(r):
            at = pl.ds(r * ROWS, ROWS)
            acc[pl.ds(ch * half + r * ROWS, ROWS), :] = ownp[ch, at, :] + pair[z, ch, at, :].astype(
                F32
            )

    for first, from_slot in ((0, z), (Z - 1, Z)):
        for step in range(2):

            @pl.when(z != first)
            def _():
                ch = half_of(z, step)
                chain_arrived(from_slot, ch)

                @pl.loop(0, half // ROWS)
                def _(r):
                    at = pl.ds(ch * half + r * ROWS, ROWS)
                    acc[at, :] = acc[at, :] + chain[from_slot, ch, pl.ds(r * ROWS, ROWS), :].astype(
                        F32
                    )

    @pl.loop(0, Wr // ROWS)
    def _(r):
        at = pl.ds(r * ROWS, ROWS)
        acc[at, :] = acc[at, :] * scale

    for ch in range(2):
        gow_copy(ch).start()

    for ch in range(2):
        pair_copy(z, ch, 0, ch).wait_send()

        @pl.when(z > 0)
        def _():
            pair_copy(z, ch, 1, ch).wait_send()

        @pl.loop(0, Z)
        def _(k):
            w_swap(k, ch).wait_send()

            @pl.when(jnp.logical_and(k <= z, z < Z - 1))
            def _():
                w_right(k, ch).wait_send()

            @pl.when(jnp.logical_and(k >= z, z > 0))
            def _():
                w_left(k, ch).wait_send()

            @pl.when(k > z)
            def _():
                chain_right(k, ch).wait_send()

            @pl.when(k < z)
            def _():
                chain_left(k, ch).wait_send()

    for sub in subs:
        if H == 4:
            g_relay(2, 1, sub, 0).wait_send()
            g_relay(1, 2, sub, 1).wait_send()
        for j in others if H != 4 else (1, 2):
            for hf in range(2):
                g_to(j, sub, hf).wait_send()
    for ch in range(2):
        gow_copy(ch).wait()


def mixer(grad_output, out_weight, ssd_out, gate, norm_weight):
    S, H = lax.axis_size("seq"), lax.axis_size("head")
    T, F = grad_output.shape
    Wr, C = out_weight.shape
    Z = S // 2
    half = Wr // 2
    nsub = F // Wr
    hbm = pl.BlockSpec(memory_space=pl.ANY)
    dma = pltpu.SemaphoreType.DMA
    flops = 4 * T * F * H * C
    gate_grad, ssd_grad, gow, _ = pl.pallas_call(
        functools.partial(mixer_kernel, (S, H, T, F, Wr, C)),
        out_shape=(
            jax.ShapeDtypeStruct((T, C), BF16),
            jax.ShapeDtypeStruct((T, C), BF16),
            jax.ShapeDtypeStruct((Wr, C), F32),
            jax.ShapeDtypeStruct((S, 2, half, C), BF16),
        ),
        in_specs=[hbm, hbm, hbm, hbm, pl.BlockSpec(memory_space=pltpu.VMEM)],
        out_specs=(hbm, hbm, hbm, hbm),
        scratch_shapes=[
            pltpu.VMEM((S, 2, T, half), BF16),
            pltpu.VMEM((T, C), BF16),
            pltpu.VMEM((T, C), F32),
            pltpu.VMEM((Z, 2, half, C), BF16),
            pltpu.VMEM((Z + 1, 2, half, C), BF16),
            pltpu.VMEM((2, 2, half, C), BF16),
            pltpu.VMEM((2, half, C), F32),
            pltpu.VMEM((Wr, T), BF16),
            pltpu.VMEM((2, 2, half, C), BF16),
            pltpu.VMEM((2, TILE_ROWS, C), BF16),
            pltpu.VMEM((2, TILE_ROWS, C), BF16),
            pltpu.VMEM((2, 2, TILE_ROWS, C), BF16),
            pltpu.VMEM((T, 128), F32),
            pltpu.VMEM((H, 8, T), F32),
            pltpu.VMEM((H, 8, T), F32),
            pltpu.VMEM((T, 128), F32),
            pltpu.VMEM((T, 128), F32),
            dma((S, 2)),
            dma((Z, 2)),
            dma((Z, 2)),
            dma((Z, 2)),
            dma((S, 2)),
            dma((H, nsub, 2)),
            dma((H,)),
            dma((H,)),
            dma((H,)),
            dma((H,)),
            dma((Z, 2)),
            dma((2, 2)),
            dma((Z + 1, 2)),
            dma((Z, 2)),
            dma((nsub, 2)),
            dma((2, 2)),
            dma((2, 2)),
            dma((2, 2)),
        ],
        compiler_params=pltpu.CompilerParams(
            collective_id=0, has_side_effects=True, vmem_limit_bytes=67043328
        ),
        cost_estimate=pl.CostEstimate(flops=flops, bytes_accessed=64 << 20, transcendentals=0),
        name="mixer",
    )(grad_output, out_weight, ssd_out, gate, norm_weight.reshape(1, C))
    return gate_grad, ssd_grad, gow


def shifted(x, axis, by):
    size = lax.axis_size(axis)
    pairs = [(i, i + by) for i in range(size) if 0 <= i + by < size]
    return lax.ppermute(x, axis, pairs)


def arriving(summary, totals, axis):
    size = lax.axis_size(axis)
    me = lax.axis_index(axis)
    pair_id, side = me // 2, me % 2
    first = side == 0
    half = summary.shape[0] // 2
    swap = [(i, i ^ 1) for i in range(size)]

    def partner(x):
        return lax.ppermute(x.astype(jnp.bfloat16), axis, swap).astype(jnp.float32)

    def mine(x):
        return lax.dynamic_slice_in_dim(x, side * half, half, 0)

    def decay(which):
        return jnp.exp(lax.dynamic_index_in_dim(totals, which, 0, keepdims=False))[:, None, None]

    other = partner(summary)
    lower = jnp.where(first, summary, other)
    upper = jnp.where(first, other, summary)
    pair = mine(lower + decay(2 * pair_id) * upper).astype(jnp.bfloat16)
    pair_totals = totals[0::2] + totals[1::2]
    order = jnp.arange(size // 2)[:, None]
    carry = jnp.zeros(pair.shape, jnp.float32)
    for hop in range(1, size // 2):
        between = (order > pair_id) & (order < pair_id + hop)
        weight = jnp.exp(jnp.sum(jnp.where(between, pair_totals, 0.0), axis=0))
        carry = carry + mine(weight)[:, None, None] * shifted(pair, axis, -2 * hop).astype(
            jnp.float32
        )
    swapped = partner(carry)
    whole = jnp.where(
        first, jnp.concatenate([carry, swapped]), jnp.concatenate([swapped, carry])
    )
    return jnp.where(first, upper + decay(2 * pair_id + 1) * whole, whole)


def on_device(
    grad_output,
    out_weight,
    ssd_out,
    gate,
    norm_weight,
    time_step,
    log_decay,
    state_in,
    state_out,
    skip,
):
    tok_rows = ssd_out.shape[0]
    local_width = ssd_out.shape[1]
    grad_gate, grad_ssd, grad_out_weight = mixer(
        grad_output, out_weight, ssd_out, gate, norm_weight
    )
    totals = lax.all_gather(jnp.sum(log_decay, axis=1), "seq", axis=0)
    heads_here = time_step.shape[0]
    head_width = local_width // heads_here
    blocks = tok_rows // BLOCK_LEN
    state_width = state_in.shape[2]
    group_count = state_in.shape[1]
    first_head = lax.axis_index("head") * heads_here
    head_ids = first_head + jnp.arange(heads_here, dtype=jnp.int32)
    group_ids = head_ids // (HEADS // GROUPS)
    group_pick = (group_ids[:, None] == jnp.arange(group_count, dtype=jnp.int32)[None, :]).astype(
        jnp.bfloat16
    )
    b_heads = jnp.einsum(
        "tgn,hg->htn", state_in, group_pick, preferred_element_type=jnp.float32
    ).astype(jnp.bfloat16)
    b_heads = b_heads.reshape(heads_here, blocks, BLOCK_LEN, state_width)
    c_heads = jnp.einsum(
        "tgn,hg->htn", state_out, group_pick, preferred_element_type=jnp.float32
    ).astype(jnp.bfloat16)
    c_heads = c_heads.reshape(heads_here, blocks, BLOCK_LEN, state_width)
    grad_heads = grad_ssd.reshape(tok_rows, heads_here, head_width).transpose(1, 0, 2)
    grad_heads = grad_heads.reshape(heads_here, blocks, BLOCK_LEN, head_width)
    cumulative = jnp.cumsum(log_decay.reshape(heads_here, blocks, BLOCK_LEN), axis=2)
    block_total = cumulative[..., -1]
    sequence_indices = jnp.arange(BLOCK_LEN)
    upper_mask = sequence_indices[None, :] >= sequence_indices[:, None]
    scores = jnp.einsum("hktn,hksn->hkts", b_heads, c_heads, preferred_element_type=jnp.float32)
    log_gap = cumulative[..., None, :] - cumulative[..., :, None]
    block_weights = jnp.where(upper_mask, scores * jnp.exp(jnp.minimum(log_gap, 0.0)), 0.0).astype(
        jnp.bfloat16
    )
    within = jnp.einsum(
        "hkts,hksp->hktp", block_weights, grad_heads, preferred_element_type=jnp.float32
    )
    within = lax.optimization_barrier(within)
    grad_float = grad_heads.astype(jnp.float32)
    scaled = (jnp.exp(cumulative)[..., None] * grad_float).astype(jnp.bfloat16)
    block_state = jnp.einsum("hksp,hksn->hkpn", scaled, c_heads, preferred_element_type=jnp.float32)

    def fold_block(carried, inputs):
        state_now, total_now = inputs
        return (state_now + jnp.exp(total_now)[:, None, None] * carried, carried)

    zero_state = jnp.zeros((heads_here, head_width, state_width), jnp.float32)
    summary, inside = lax.scan(
        fold_block, zero_state, (block_state.transpose(1, 0, 2, 3), block_total.T), reverse=True
    )
    tail_decay = jnp.exp(
        jnp.sum(block_total, axis=1, keepdims=True) - jnp.cumsum(block_total, axis=1)
    )

    remote = arriving(summary, totals, "seq")
    full_states = inside.transpose(1, 0, 2, 3) + tail_decay[..., None, None] * remote[:, None]
    carry_low = full_states.astype(jnp.bfloat16)
    across = jnp.einsum("hkpn,hktn->hktp", carry_low, b_heads, preferred_element_type=jnp.float32)
    across = across * jnp.exp(block_total[..., None] - cumulative)[..., None]
    step_sizes = time_step.reshape(heads_here, blocks, BLOCK_LEN)
    grad_head = step_sizes[..., None] * (within + across) + skip[:, None, None, None] * grad_float
    grad_x = (
        grad_head.reshape(heads_here, tok_rows, head_width)
        .transpose(1, 0, 2)
        .reshape(tok_rows, local_width)
    )
    return (grad_x.astype(jnp.bfloat16), grad_gate, grad_out_weight)


def solution(mesh):
    return jax.shard_map(
        on_device,
        mesh=mesh,
        in_specs=(
            P("seq", "head"),
            P("seq", "head"),
            P("seq", "head"),
            P("seq", "head"),
            P("head"),
            P("head", "seq"),
            P("head", "seq"),
            P("seq", None, None),
            P("seq", None, None),
            P("head"),
        ),
        out_specs=(P("seq", "head"), P("seq", "head"), P("seq", "head")),
        check_vma=False,
    )
```

```python
import functools
import math

import jax
import jax.numpy as jnp
from jax import lax
from jax.experimental import pallas as pl
from jax.experimental.pallas import tpu as pltpu
from jax.sharding import PartitionSpec as P

HEADS = 128
GROUPS = 8
BLOCK_LEN = 256
MESH = pl.DeviceIdType.MESH
F32 = jnp.float32
BF16 = jnp.bfloat16
ROWS = 16
TILE_ROWS = 64
CHUNK = 128


epsilon = 1e-05


def remote(src, dst, send_sem, recv_sem, **device):
    return pltpu.make_async_remote_copy(
        src_ref=src,
        dst_ref=dst,
        send_sem=send_sem,
        recv_sem=recv_sem,
        device_id=device,
        device_id_type=MESH,
    )


def lane_sum(x):
    total = x[:, 0:128]
    for j in range(1, x.shape[1] // 128):
        total = total + x[:, j * 128 : (j + 1) * 128]
    return total


def mixer_kernel(
    dims,
    g_ref,
    w_ref,
    y_ref,
    z_ref,
    nw_ref,
    ts_ref,
    ld_ref,
    b_ref,
    c_ref,
    skip_ref,
    gate_out,
    gx_out,
    gow_out,
    wfull,
    gfull,
    nbuf,
    acc,
    pair,
    chain,
    pst,
    ownp,
    gt,
    wbuf,
    ybuf,
    zbuf,
    obuf,
    sqp,
    sqx,
    wgx,
    invc,
    cfc,
    cum_row,
    cum_col,
    spread,
    run,
    summ,
    decay,
    rbuf,
    vbuf,
    arrived,
    ag_recv,
    ag_r,
    ag_l,
    ag_p,
    g_recv,
    g_send,
    sq_recv,
    sq_send,
    wg_recv,
    wg_send,
    pair_recv,
    pair_send,
    ch_recv,
    ch_send,
    loc,
    wsem,
    in_sem,
    out_sem,
    swap_recv,
    swap_send,
    st_recv,
    st_send,
    half_recv,
    half_send,
):
    S, H, T, F, Wr, C = dims
    Z = S // 2
    half = Wr // 2
    nsub = F // Wr
    DI = C * H
    TN = min(256, C)
    HL = ld_ref.shape[0]
    HD = C // HL
    GW = min(C, (HEADS // GROUPS) * HD)
    NG = C // GW
    HPG = GW // HD
    NS = b_ref.shape[2]
    CH = C // 2
    chunks = T // CHUNK
    PARTS = 4
    s = lax.axis_index("seq")
    h = lax.axis_index("head")
    z = s // 2
    c = s % 2
    zm = Z - 1 - z
    partner = s + 1 - 2 * c
    others = range(1, H)

    barrier = pltpu.get_barrier_semaphore()
    pl.semaphore_signal(barrier, inc=1, device_id={"seq": partner}, device_id_type=MESH)
    for j in others:
        pl.semaphore_signal(barrier, inc=1, device_id={"head": h ^ j}, device_id_type=MESH)

    @pl.when(z > 0)
    def _():
        pl.semaphore_signal(barrier, inc=1, device_id={"seq": s - 2}, device_id_type=MESH)

    @pl.when(z < Z - 1)
    def _():
        pl.semaphore_signal(barrier, inc=1, device_id={"seq": s + 2}, device_id_type=MESH)

    peers = H + jnp.where(z > 0, 1, 0) + jnp.where(z < Z - 1, 1, 0)
    pl.semaphore_wait(barrier, peers)

    def w_src(k, ch, own):
        return w_ref.at[pl.ds(ch * half, half)] if own else wfull.at[2 * k + c, ch]

    def w_right(k, ch, own=False):
        q = 2 * k + c
        return remote(
            w_src(k, ch, own), wfull.at[q, ch], ag_r.at[k, ch], ag_recv.at[q, ch], seq=s + 2
        )

    def w_left(k, ch, own=False):
        q = 2 * k + c
        return remote(
            w_src(k, ch, own), wfull.at[q, ch], ag_l.at[k, ch], ag_recv.at[q, ch], seq=s - 2
        )

    def w_swap(k, ch, own=False):
        q = 2 * k + c
        return remote(
            w_src(k, ch, own), wfull.at[q, ch], ag_p.at[k, ch], ag_recv.at[q, ch], seq=partner
        )

    def w_arrived(q, ch):
        remote(
            wfull.at[q, ch], wfull.at[q, ch], ag_p.at[0, 0], ag_recv.at[q, ch], seq=partner
        ).wait_recv()

    for ch in range(2):

        @pl.when(z < Z - 1)
        def _():
            w_right(z, ch, True).start()

        @pl.when(z > 0)
        def _():
            w_left(z, ch, True).start()

        w_swap(z, ch, True).start()

    def g_own(sub, hf):
        return g_ref.at[:, pl.ds(sub * Wr + hf * half, half)]

    def g_local(sub, hf):
        return pltpu.make_async_copy(
            g_own(sub, hf), gfull.at[h * nsub + sub, hf], loc.at[sub, hf]
        )

    for sub in range(nsub):
        for hf in range(2):
            g_local(sub, hf).start()

    tiles = T // TILE_ROWS

    def fetch(t, slot):
        rows = pl.ds(t * TILE_ROWS, TILE_ROWS)
        return (
            pltpu.make_async_copy(y_ref.at[rows], ybuf.at[slot], in_sem.at[0, slot]),
            pltpu.make_async_copy(z_ref.at[rows], zbuf.at[slot], in_sem.at[1, slot]),
        )

    def stream(body):
        for copy in fetch(0, 0):
            copy.start()

        @pl.loop(0, tiles)
        def _(t):
            slot = t % 2

            @pl.when(t + 1 < tiles)
            def _():
                for copy in fetch(t + 1, 1 - slot):
                    copy.start()

            for copy in fetch(t, slot):
                copy.wait()
            body(t, slot)

    def square_tile(t, slot):
        @pl.loop(0, TILE_ROWS // ROWS)
        def _(r):
            rows = pl.ds(r * ROWS, ROWS)
            at = pl.ds(t * TILE_ROWS + r * ROWS, ROWS)
            gv = zbuf[slot, rows, :].astype(F32)
            gated = ybuf[slot, rows, :].astype(F32) * (gv * jax.nn.sigmoid(gv))
            acc[at, :] = gated
            sqp[at, :] = lane_sum(gated * gated)

    stream(square_tile)

    def share(buf, send, recv):
        buf[h] = jnp.broadcast_to(jnp.sum(sqp[...].T, axis=0, keepdims=True), (8, T))
        for j in others:
            remote(buf.at[h], buf.at[h], send.at[j], recv.at[h], head=h ^ j).start()

    def shared(buf, send, recv):
        for j in others:
            remote(buf.at[h ^ j], buf.at[h ^ j], send.at[j], recv.at[h ^ j], head=h ^ j).wait_recv()
        total = buf[0, 0:1, :]
        for j in others:
            total = total + buf[j, 0:1, :]
        for j in others:
            remote(buf.at[h], buf.at[h], send.at[j], recv.at[h], head=h ^ j).wait_send()
        return total

    share(sqx, sq_send, sq_recv)

    def g_to(j, sub, hf):
        q = h * nsub + sub
        return remote(
            g_own(sub, hf), gfull.at[q, hf], g_send.at[j, sub, hf], g_recv.at[q, hf], head=h ^ j
        )

    def g_relay(j, frm, sub, hf):
        q = (h ^ frm) * nsub + sub
        return remote(
            gfull.at[q, hf], gfull.at[q, hf], g_send.at[3, sub, hf], g_recv.at[q, hf], head=h ^ j
        )

    def g_arrived(j, sub, hf):
        q = (h ^ j) * nsub + sub
        remote(
            gfull.at[q, hf], gfull.at[q, hf], g_send.at[j, sub, hf], g_recv.at[q, hf], head=h ^ j
        ).wait_recv()

    subs = range(nsub)
    if H == 4:
        for sub in subs:
            g_to(1, sub, 0).start()
            g_to(2, sub, 1).start()
    else:
        for j in others:
            for sub in subs:
                for hf in range(2):
                    g_to(j, sub, hf).start()

    inv_row = lax.rsqrt(shared(sqx, sq_send, sq_recv) / DI + epsilon)
    invc[...] = jnp.broadcast_to(inv_row, (128, T)).T

    @pl.loop(0, T // ROWS)
    def _(r):
        at = pl.ds(r * ROWS, ROWS)
        nbuf[at, :] = (acc[at, :] * invc[at, 0:1] * nw_ref[...]).astype(BF16)

    for sub in subs:
        for hf in range(2):
            g_local(sub, hf).wait()
    if H == 4:
        for sub in subs:
            g_arrived(1, sub, 0)
            g_relay(2, 1, sub, 0).start()
        for sub in subs:
            g_arrived(2, sub, 1)
            g_relay(1, 2, sub, 1).start()
        for sub in subs:
            g_to(1, sub, 1).start()
            g_to(2, sub, 0).start()


    tri = (
        lax.broadcasted_iota(jnp.int32, (CHUNK, CHUNK), 0)
        <= lax.broadcasted_iota(jnp.int32, (CHUNK, CHUNK), 1)
    ).astype(F32)
    cum_row[...] = jnp.zeros_like(cum_row)
    for q in range(chunks):
        cols = slice(q * CHUNK, (q + 1) * CHUNK)
        cum_row[0:HL, cols] = jnp.dot(
            ld_ref[:, cols], tri, precision=lax.Precision.HIGHEST, preferred_element_type=F32
        )
    cum_col[...] = cum_row[...].T
    spread[...] = (
        lax.broadcasted_iota(jnp.int32, (128, C), 0)
        == lax.broadcasted_iota(jnp.int32, (128, C), 1) // HD
    ).astype(BF16)

    def widen(x, g):
        high = x.astype(BF16)
        low = (x - high.astype(F32)).astype(BF16)
        onto = spread[:, g * GW : (g + 1) * GW]
        return jnp.dot(high, onto, preferred_element_type=F32) + jnp.dot(
            low, onto, preferred_element_type=F32
        )

    def last_of(q):
        return cum_col[pl.ds(q * CHUNK + CHUNK - 1, 1), :]

    def pair_copy(k, cx, d, ch):
        return remote(
            pst.at[d, ch], pair.at[k, cx], pair_send.at[d, ch], pair_recv.at[k, cx], seq=partner
        )

    def rs_prep(k, cx, d, ch, slot):
        gt[0:half, :] = gfull[2 * k + 1 - c, cx].T
        gt[half:Wr, :] = gfull[2 * k + c, cx].T

        @pl.loop(0, C // TN)
        def _(t):
            cols = pl.ds(pl.multiple_of(t * TN, TN), TN)
            part = jnp.dot(gt[...], nbuf[:, cols], preferred_element_type=F32)
            pst[d, ch, :, cols] = part[:half].astype(BF16)
            ownp[slot, :, cols] = part[half:]

        pair_copy(k, cx, d, ch).start()

    def chain_right(k, cx):
        return remote(
            chain.at[k, cx], chain.at[k, cx], ch_send.at[k, cx], ch_recv.at[k, cx], seq=s + 2
        )

    def chain_left(k, cx):
        to = jnp.where(k == z - 1, Z, k)
        return remote(
            chain.at[k, cx], chain.at[to, cx], ch_send.at[k, cx], ch_recv.at[to, cx], seq=s - 2
        )

    def chain_arrived(k, cx):
        remote(
            chain.at[k, cx], chain.at[k, cx], ch_send.at[0, 0], ch_recv.at[k, cx], seq=partner
        ).wait_recv()

    def rs_sum(k, cx, d, ch, chained):
        pair_copy(k, cx, d, ch).wait_recv()

        @pl.when(chained)
        def _():
            chain_arrived(k, cx)

            @pl.loop(0, half // ROWS)
            def _(r):
                at = pl.ds(r * ROWS, ROWS)
                chain[k, cx, at, :] = (
                    ownp[d, at, :] + pair[k, cx, at, :].astype(F32) + chain[k, cx, at, :].astype(F32)
                ).astype(BF16)

        @pl.when(jnp.logical_not(chained))
        def _():
            @pl.loop(0, half // ROWS)
            def _(r):
                at = pl.ds(r * ROWS, ROWS)
                chain[k, cx, at, :] = (ownp[d, at, :] + pair[k, cx, at, :].astype(F32)).astype(BF16)

    def half_of(k, ch):
        if H != 4:
            return ch
        return jnp.where((2 * k * Wr // F) ^ h == 2, 1 - ch, ch)

    near = jnp.minimum(z, zm)

    def plane_of(p):
        d = (p + 1) // 2
        close = jnp.where(p % 2 == 1, z - d, z + d)
        far = jnp.where(z < zm, z + (p - near), z - (p - near))
        return jnp.where(p <= 2 * near, close, far)

    def w_load(src, par, ch):
        return pltpu.make_async_copy(src, wbuf.at[par, ch], wsem.at[par, ch])

    def project(p, first):
        k = plane_of(p)
        for ch in range(2):
            w_arrived(2 * k + 1 - c, ch)
        for par in range(2):
            for ch in range(2):
                mine = jnp.logical_and(k == z, c == par)

                @pl.when(mine)
                def _():
                    w_load(w_ref.at[pl.ds(ch * half, half)], par, ch).start()

                @pl.when(jnp.logical_not(mine))
                def _():
                    w_load(wfull.at[2 * k + par, ch], par, ch).start()

        for par in range(2):
            for ch in range(2):
                w_load(wfull.at[2 * k + par, ch], par, ch).wait()

        @pl.loop(0, C // TN)
        def _(t):
            cols = pl.ds(pl.multiple_of(t * TN, TN), TN)
            total = None if first else acc[:, cols]
            for par in range(2):
                for ch in range(2):
                    part = jnp.dot(
                        gfull[2 * k + par, ch], wbuf[par, ch, :, cols], preferred_element_type=F32
                    )
                    total = part if total is None else total + part
            acc[:, cols] = total

    @pl.loop(2, 2 * Z)
    def _(i):
        slot = i // 2
        ch = i % 2

        @pl.when(z - slot >= 0)
        def _():
            k = z - slot
            w_arrived(2 * k + c, ch)

            @pl.when(z < Z - 1)
            def _():
                w_right(k, ch).start()

            w_swap(k, ch).start()

        @pl.when(z + slot <= Z - 1)
        def _():
            k = z + slot
            w_arrived(2 * k + c, ch)

            @pl.when(z > 0)
            def _():
                w_left(k, ch).start()

            w_swap(k, ch).start()

        @pl.when(i == 2)
        def _():
            for j in (others if H != 4 else (3,)):
                for sub in subs:
                    for hf in range(2):
                        g_arrived(j, sub, hf)

        if H == 4:

            @pl.when(i == 3)
            def _():
                for sub in subs:
                    g_arrived(1, sub, 1)
                    g_arrived(2, sub, 0)

        go_right = jnp.logical_and(slot > z, z < Z - 1)
        go_left = jnp.logical_and(slot > zm, z > 0)
        kr = Z + z - slot
        kl = slot - Z + z

        @pl.when(go_right)
        def _():
            @pl.when(slot - 1 > z)
            def _():
                pair_copy(kr, 0, 0, ch).wait_send()

            rs_prep(kr, half_of(kr, ch), 0, ch, 0)

        @pl.when(go_left)
        def _():
            @pl.when(slot - 1 > zm)
            def _():
                pair_copy(kl, 0, 1, ch).wait_send()

            rs_prep(kl, half_of(kl, ch), 1, ch, 1)

        @pl.when(go_right)
        def _():
            cx = half_of(kr, ch)
            rs_sum(kr, cx, 0, ch, z > 0)
            chain_right(kr, cx).start()

        @pl.when(go_left)
        def _():
            cx = half_of(kl, ch)
            rs_sum(kl, cx, 1, ch, z < Z - 1)
            chain_left(kl, cx).start()

        @pl.when(i == 4)
        def _():
            project(0, True)

        lo = jnp.where(i == 4, 1, jnp.where(i == 5, 2, slot))
        hi = jnp.where(
            i == 4, 2, jnp.where(i == 5, 3, jnp.where((slot >= 3) & (ch == 1), slot + 1, slot))
        )
        hi = jnp.where(i < 4, lo, jnp.minimum(hi, Z - 1))

        @pl.loop(lo, hi)
        def _(p):
            project(p, False)

    project(Z - 1, False)

    @pl.loop(0, T // ROWS)
    def _(r):
        at = pl.ds(r * ROWS, ROWS)
        sqp[at, :] = lane_sum(acc[at, :] * nbuf[at, :].astype(F32))

    share(wgx, wg_send, wg_recv)
    for ch in range(2):

        @pl.when(Z - 1 > z)
        def _():
            pair_copy(z, ch, 0, ch).wait_send()

        rs_prep(z, ch, 0, ch, ch)

    weighted = shared(wgx, wg_send, wg_recv) / DI
    cfc[...] = jnp.broadcast_to(weighted, (128, T)).T * invc[...] * invc[...]

    def put(t, slot):
        rows = pl.ds(t * TILE_ROWS, TILE_ROWS)
        return pltpu.make_async_copy(obuf.at[slot], gate_out.at[rows], out_sem.at[0, slot])

    def grad_tile(t, slot):
        @pl.when(t >= 2)
        def _():
            put(t - 2, slot).wait()

        @pl.loop(0, TILE_ROWS // ROWS)
        def _(r):
            rows = pl.ds(r * ROWS, ROWS)
            at = pl.ds(t * TILE_ROWS + r * ROWS, ROWS)
            gv = zbuf[slot, rows, :].astype(F32)
            values = ybuf[slot, rows, :].astype(F32)
            sig = jax.nn.sigmoid(gv)
            silu = gv * sig
            gg = invc[at, 0:1] * nw_ref[...] * acc[at, :] - values * silu * cfc[at, 0:1]
            obuf[slot, rows, :] = (gg * values * sig * (1.0 + gv * (1.0 - sig))).astype(BF16)
            nbuf[at, :] = (gg * silu).astype(BF16)

        put(t, slot).start()

    stream(grad_tile)
    for t in (tiles - 2, tiles - 1):
        put(t, t % 2).wait()

    pads = jnp.zeros((128 - HL, T), F32)
    cfc[...] = jnp.concatenate([ts_ref[...], pads], axis=0).T
    per = 2 * half // CHUNK

    def inside(q):
        plane = lax.rem(z + 1 + q // per, Z)
        r = q % per
        rows = half // CHUNK
        return plane, r // rows, pl.ds(pl.multiple_of((r % rows) * CHUNK, CHUNK), CHUNK)

    run[...] = jnp.zeros_like(run)

    @pl.loop(0, chunks, init_carry=jnp.zeros((1, 128), F32))
    def tail(step, later):
        q = chunks - 1 - step
        at = pl.ds(pl.multiple_of(q * CHUNK, CHUNK), CHUNK)
        total = last_of(q)
        sqp[at, :] = total - cum_col[at, :] + later
        grow = jnp.exp(cum_col[at, :])
        keep = jnp.exp(jnp.broadcast_to(total, (8, 128)))
        plane, hf, rows = inside(q)
        for g in range(NG):
            cols = slice(g * GW, (g + 1) * GW)
            scaled = (widen(grow, g) * nbuf[at, cols].astype(F32)).astype(BF16)
            state = jnp.dot(c_ref[g, at, :].T, scaled, preferred_element_type=F32)
            pair[plane, hf, rows, cols] = run[:, cols].astype(BF16)
            run[:, cols] = state + widen(keep, g)[0:1, :] * run[:, cols]
        return later + total

    summ[c] = run[...].astype(BF16)
    keep_all = jnp.exp(jnp.broadcast_to(tail, (8, 128)))
    for g in range(NG):
        decay[c, :, g * GW : (g + 1) * GW] = widen(keep_all, g)

    def swaps():
        return (
            remote(summ.at[c], summ.at[c], swap_send.at[0], swap_recv.at[0], seq=partner),
            remote(decay.at[c], decay.at[c], swap_send.at[1], swap_recv.at[1], seq=partner),
        )

    for copy in swaps():
        copy.start()

    def state_left(part):
        rows = pl.ds(part * (NS // PARTS), NS // PARTS)
        return remote(
            vbuf.at[rows], rbuf.at[c, rows], st_send.at[part], st_recv.at[part], seq=s - 2
        )

    def state_swap(part):
        rows = pl.ds(part * (NS // PARTS), NS // PARTS)
        return remote(
            rbuf.at[c, rows], rbuf.at[c, rows], half_send.at[part], half_recv.at[part], seq=partner
        )

    mine_cols = pl.ds(pl.multiple_of(c * CH, CH), CH)

    def state_step(part):
        rows = pl.ds(part * (NS // PARTS), NS // PARTS)

        @pl.when(z < Z - 1)
        def _():
            state_left(part).wait_recv()
            state_swap(part).start()

        @pl.when(z > 0)
        def _():
            first_keep = decay[0, 0:1, mine_cols]
            here = summ[0, rows, mine_cols].astype(F32) + first_keep * summ[
                1, rows, mine_cols
            ].astype(F32)

            @pl.when(z < Z - 1)
            def _():
                vbuf[rows, :] = (
                    here
                    + first_keep * decay[1, 0:1, mine_cols] * rbuf[c, rows, :].astype(F32)
                ).astype(BF16)

            @pl.when(z == Z - 1)
            def _():
                vbuf[rows, :] = here.astype(BF16)

            state_left(part).start()

    upper = lax.broadcasted_iota(jnp.int32, (CHUNK, CHUNK), 1) >= lax.broadcasted_iota(
        jnp.int32, (CHUNK, CHUNK), 0
    )
    lane = lax.broadcasted_iota(jnp.int32, (CHUNK, 2 * HD), 1)

    @pl.loop(0, chunks)
    def _(q):
        @pl.when(q == 0)
        def _():
            for copy in swaps():
                copy.wait_recv()

        for part in range(PARTS):

            @pl.when(q == jnp.minimum(zm + part, chunks - 1))
            def _():
                state_step(part)

        at = pl.ds(pl.multiple_of(q * CHUNK, CHUNK), CHUNK)
        plane, hf, rows = inside(q)
        cum = cum_col[at, :]
        fade = jnp.exp(last_of(q) - cum)
        steps = cfc[at, :]
        skips = jnp.broadcast_to(skip_ref[...], (8, 128))
        for g in range(NG):
            b = b_ref[g, at, :]
            scores = lax.dot_general(
                b, c_ref[g, at, :], (((1,), (1,)), ((), ())), preferred_element_type=F32
            )
            scores = jnp.where(upper, scores, 0.0)
            cols = slice(g * GW, (g + 1) * GW)
            acc[at, cols] = widen(fade, g) * jnp.dot(
                b, pair[plane, hf, rows, cols], preferred_element_type=F32
            )
            for j in range(HPG // 2):
                weights = []
                for head in (g * HPG + 2 * j, g * HPG + 2 * j + 1):
                    gap = cum_row[head : head + 1, at] - cum[:, head : head + 1]
                    weights.append((scores * jnp.exp(jnp.minimum(gap, 0.0))).astype(BF16))
                span = slice(g * GW + 2 * j * HD, g * GW + 2 * (j + 1) * HD)
                both = nbuf[at, span]
                zero = jnp.zeros_like(both)
                stacked = jnp.concatenate(
                    [jnp.where(lane < HD, both, zero), jnp.where(lane < HD, zero, both)], axis=0
                )
                acc[at, span] = acc[at, span] + jnp.dot(
                    jnp.concatenate(weights, axis=1), stacked, preferred_element_type=F32
                )
            acc[at, cols] = widen(steps, g) * acc[at, cols] + widen(skips, g)[0:1, :] * nbuf[
                at, cols
            ].astype(F32)

    @pl.when(z < Z - 1)
    def _():
        for part in range(PARTS):
            rows = pl.ds(part * (NS // PARTS), NS // PARTS)
            remote(
                rbuf.at[1 - c, rows],
                rbuf.at[1 - c, rows],
                half_send.at[part],
                half_recv.at[part],
                seq=partner,
            ).wait_recv()

    @pl.when(z == Z - 1)
    def _():
        rbuf[...] = jnp.zeros_like(rbuf)

    for side in range(2):
        cols = slice(side * CH, (side + 1) * CH)
        later = rbuf[side].astype(F32)

        @pl.when(c == 1)
        def _():
            arrived[:, cols] = later.astype(BF16)

        @pl.when(c == 0)
        def _():
            arrived[:, cols] = (
                summ[1, :, cols].astype(F32) + decay[1, 0:1, cols] * later
            ).astype(BF16)

    def put_x(t, slot):
        rows = pl.ds(t * TILE_ROWS, TILE_ROWS)
        return pltpu.make_async_copy(ybuf.at[slot], gx_out.at[rows], out_sem.at[1, slot])

    @pl.loop(0, tiles)
    def _(t):
        slot = t % 2
        at = pl.ds(pl.multiple_of(t * TILE_ROWS, TILE_ROWS), TILE_ROWS)

        @pl.when(t >= 2)
        def _():
            put_x(t - 2, slot).wait()

        factor = cfc[at, :] * jnp.exp(sqp[at, :])
        for g in range(NG):
            cols = slice(g * GW, (g + 1) * GW)
            ybuf[slot, :, cols] = (
                acc[at, cols]
                + widen(factor, g)
                * jnp.dot(b_ref[g, at, :], arrived[:, cols], preferred_element_type=F32)
            ).astype(BF16)
        put_x(t, slot).start()

    scale = 1.0 / math.sqrt(T * S)

    def gow_copy(ch):
        rows = pl.ds(ch * half, half)
        return pltpu.make_async_copy(ownp.at[ch], gow_out.at[rows], out_sem.at[0, ch])

    for ch in range(2):
        pair_copy(z, ch, 0, ch).wait_recv()

        @pl.loop(0, half // ROWS)
        def _(r):
            at = pl.ds(r * ROWS, ROWS)
            ownp[ch, at, :] = ownp[ch, at, :] + pair[z, ch, at, :].astype(F32)

    for first, from_slot in ((0, z), (Z - 1, Z)):
        for step in range(2):

            @pl.when(z != first)
            def _():
                ch = half_of(z, step)
                chain_arrived(from_slot, ch)

                @pl.loop(0, half // ROWS)
                def _(r):
                    at = pl.ds(r * ROWS, ROWS)
                    ownp[ch, at, :] = ownp[ch, at, :] + chain[from_slot, ch, at, :].astype(F32)

    for ch in range(2):

        @pl.loop(0, half // ROWS)
        def _(r):
            at = pl.ds(r * ROWS, ROWS)
            ownp[ch, at, :] = ownp[ch, at, :] * scale

        gow_copy(ch).start()

    for t in (tiles - 2, tiles - 1):
        put_x(t, t % 2).wait()

    for copy in swaps():
        copy.wait_send()
    for part in range(PARTS):

        @pl.when(z < Z - 1)
        def _():
            state_swap(part).wait_send()

        @pl.when(z > 0)
        def _():
            state_left(part).wait_send()

    for ch in range(2):
        pair_copy(z, ch, 0, ch).wait_send()

        @pl.when(z > 0)
        def _():
            pair_copy(z, ch, 1, ch).wait_send()

        @pl.loop(0, Z)
        def _(k):
            w_swap(k, ch).wait_send()

            @pl.when(jnp.logical_and(k <= z, z < Z - 1))
            def _():
                w_right(k, ch).wait_send()

            @pl.when(jnp.logical_and(k >= z, z > 0))
            def _():
                w_left(k, ch).wait_send()

            @pl.when(k > z)
            def _():
                chain_right(k, ch).wait_send()

            @pl.when(k < z)
            def _():
                chain_left(k, ch).wait_send()

    for sub in subs:
        if H == 4:
            g_relay(2, 1, sub, 0).wait_send()
            g_relay(1, 2, sub, 1).wait_send()
        for j in others if H != 4 else (1, 2):
            for hf in range(2):
                g_to(j, sub, hf).wait_send()
    for ch in range(2):
        gow_copy(ch).wait()


def mixer(
    grad_output,
    out_weight,
    ssd_out,
    gate,
    norm_weight,
    time_step,
    log_decay,
    state_in,
    state_out,
    skip,
):
    S, H = lax.axis_size("seq"), lax.axis_size("head")
    T, F = grad_output.shape
    Wr, C = out_weight.shape
    Z = S // 2
    half = Wr // 2
    nsub = F // Wr
    heads_here = time_step.shape[0]
    groups_here = max(1, heads_here * GROUPS // HEADS)
    first_group = lax.axis_index("head") * heads_here // (HEADS // GROUPS)

    def picked(x):
        return lax.dynamic_slice_in_dim(x, first_group, groups_here, 1).transpose(1, 0, 2)

    skip_row = jnp.pad(skip, (0, 128 - heads_here)).reshape(1, 128)
    NS = state_in.shape[2]
    hbm = pl.BlockSpec(memory_space=pl.ANY)
    vmem = pl.BlockSpec(memory_space=pltpu.VMEM)
    dma = pltpu.SemaphoreType.DMA
    flops = 4 * T * F * H * C
    outs = pl.pallas_call(
        functools.partial(mixer_kernel, (S, H, T, F, Wr, C)),
        out_shape=(
            jax.ShapeDtypeStruct((T, C), BF16),
            jax.ShapeDtypeStruct((T, C), BF16),
            jax.ShapeDtypeStruct((Wr, C), F32),
            jax.ShapeDtypeStruct((S, 2, half, C), BF16),
        ),
        in_specs=[hbm] * 4 + [vmem] * 6,
        out_specs=(hbm,) * 4,
        scratch_shapes=[
            pltpu.VMEM((S, 2, T, half), BF16),
            pltpu.VMEM((T, C), BF16),
            pltpu.VMEM((T, C), F32),
            pltpu.VMEM((Z, 2, half, C), BF16),
            pltpu.VMEM((Z + 1, 2, half, C), BF16),
            pltpu.VMEM((2, 2, half, C), BF16),
            pltpu.VMEM((2, half, C), F32),
            pltpu.VMEM((Wr, T), BF16),
            pltpu.VMEM((2, 2, half, C), BF16),
            pltpu.VMEM((2, TILE_ROWS, C), BF16),
            pltpu.VMEM((2, TILE_ROWS, C), BF16),
            pltpu.VMEM((2, TILE_ROWS, C), BF16),
            pltpu.VMEM((T, 128), F32),
            pltpu.VMEM((H, 8, T), F32),
            pltpu.VMEM((H, 8, T), F32),
            pltpu.VMEM((T, 128), F32),
            pltpu.VMEM((T, 128), F32),
            pltpu.VMEM((128, T), F32),
            pltpu.VMEM((T, 128), F32),
            pltpu.VMEM((128, C), BF16),
            pltpu.VMEM((NS, C), F32),
            pltpu.VMEM((2, NS, C), BF16),
            pltpu.VMEM((2, 8, C), F32),
            pltpu.VMEM((2, NS, C // 2), BF16),
            pltpu.VMEM((NS, C // 2), BF16),
            pltpu.VMEM((NS, C), BF16),
            dma((S, 2)),
            dma((Z, 2)),
            dma((Z, 2)),
            dma((Z, 2)),
            dma((S, 2)),
            dma((H, nsub, 2)),
            dma((H,)),
            dma((H,)),
            dma((H,)),
            dma((H,)),
            dma((Z, 2)),
            dma((2, 2)),
            dma((Z + 1, 2)),
            dma((Z, 2)),
            dma((nsub, 2)),
            dma((2, 2)),
            dma((2, 2)),
            dma((2, 2)),
            dma((2,)),
            dma((2,)),
            dma((4,)),
            dma((4,)),
            dma((4,)),
            dma((4,)),
        ],
        compiler_params=pltpu.CompilerParams(
            collective_id=0, has_side_effects=True, vmem_limit_bytes=67043328
        ),
        cost_estimate=pl.CostEstimate(flops=flops, bytes_accessed=64 << 20, transcendentals=0),
        name="mixer",
    )(
        grad_output,
        out_weight,
        ssd_out,
        gate,
        norm_weight.reshape(1, C),
        time_step,
        log_decay,
        picked(state_in),
        picked(state_out),
        skip_row,
    )
    grad_gate, grad_x, grad_out_weight, _ = outs
    return grad_x, grad_gate, grad_out_weight


def solution(mesh):
    return jax.shard_map(
        mixer,
        mesh=mesh,
        in_specs=(
            P("seq", "head"),
            P("seq", "head"),
            P("seq", "head"),
            P("seq", "head"),
            P("head"),
            P("head", "seq"),
            P("head", "seq"),
            P("seq", None, None),
            P("seq", None, None),
            P("head"),
        ),
        out_specs=(P("seq", "head"), P("seq", "head"), P("seq", "head")),
        check_vma=False,
    )
```

```python
import functools
import math

import jax
import jax.numpy as jnp
from jax import lax
from jax.experimental import pallas as pl
from jax.experimental.pallas import tpu as pltpu
from jax.sharding import PartitionSpec as P

HEADS = 128
GROUPS = 8
BLOCK_LEN = 256
MESH = pl.DeviceIdType.MESH
F32 = jnp.float32
BF16 = jnp.bfloat16
ROWS = 16
TILE_ROWS = 64
CHUNK = 128


epsilon = 1e-05


def remote(src, dst, send_sem, recv_sem, **device):
    return pltpu.make_async_remote_copy(
        src_ref=src,
        dst_ref=dst,
        send_sem=send_sem,
        recv_sem=recv_sem,
        device_id=device,
        device_id_type=MESH,
    )


def lane_sum(x):
    total = x[:, 0:128]
    for j in range(1, x.shape[1] // 128):
        total = total + x[:, j * 128 : (j + 1) * 128]
    return total


def mixer_kernel(
    dims,
    g_ref,
    w_ref,
    y_ref,
    z_ref,
    nw_ref,
    ts_ref,
    ld_ref,
    si_ref,
    so_ref,
    skip_ref,
    gate_out,
    gx_out,
    gow_out,
    wfull,
    gfull,
    nbuf,
    acc,
    pair,
    chain,
    pst,
    ownp,
    gt,
    wbuf,
    ybuf,
    zbuf,
    obuf,
    sqp,
    sqx,
    wgx,
    invc,
    cfc,
    cum_row,
    cum_col,
    spread,
    run,
    summ,
    decay,
    rbuf,
    vbuf,
    arrived,
    raw,
    b_ref,
    c_ref,
    ag_recv,
    ag_r,
    ag_l,
    ag_p,
    g_recv,
    g_send,
    sq_recv,
    sq_send,
    wg_recv,
    wg_send,
    pair_recv,
    pair_send,
    ch_recv,
    ch_send,
    loc,
    wsem,
    in_sem,
    out_sem,
    swap_recv,
    swap_send,
    st_recv,
    st_send,
    half_recv,
    half_send,
    late_sem,
):
    S, H, T, F, Wr, C = dims
    Z = S // 2
    half = Wr // 2
    nsub = F // Wr
    DI = C * H
    TN = min(256, C)
    HL = ld_ref.shape[0]
    HD = C // HL
    GW = min(C, (HEADS // GROUPS) * HD)
    NG = C // GW
    HPG = GW // HD
    NS = si_ref.shape[2]
    CH = C // 2
    chunks = T // CHUNK
    PARTS = 4
    s = lax.axis_index("seq")
    h = lax.axis_index("head")
    z = s // 2
    c = s % 2
    zm = Z - 1 - z
    first_group = h * HL // (HEADS // GROUPS)
    partner = s + 1 - 2 * c
    others = range(1, H)

    barrier = pltpu.get_barrier_semaphore()
    pl.semaphore_signal(barrier, inc=1, device_id={"seq": partner}, device_id_type=MESH)
    for j in others:
        pl.semaphore_signal(barrier, inc=1, device_id={"head": h ^ j}, device_id_type=MESH)

    @pl.when(z > 0)
    def _():
        pl.semaphore_signal(barrier, inc=1, device_id={"seq": s - 2}, device_id_type=MESH)

    @pl.when(z < Z - 1)
    def _():
        pl.semaphore_signal(barrier, inc=1, device_id={"seq": s + 2}, device_id_type=MESH)

    peers = H + jnp.where(z > 0, 1, 0) + jnp.where(z < Z - 1, 1, 0)
    pl.semaphore_wait(barrier, peers)

    def w_src(k, ch, own):
        return w_ref.at[pl.ds(ch * half, half)] if own else wfull.at[2 * k + c, ch]

    def w_right(k, ch, own=False):
        q = 2 * k + c
        return remote(
            w_src(k, ch, own), wfull.at[q, ch], ag_r.at[k, ch], ag_recv.at[q, ch], seq=s + 2
        )

    def w_left(k, ch, own=False):
        q = 2 * k + c
        return remote(
            w_src(k, ch, own), wfull.at[q, ch], ag_l.at[k, ch], ag_recv.at[q, ch], seq=s - 2
        )

    def w_swap(k, ch, own=False):
        q = 2 * k + c
        return remote(
            w_src(k, ch, own), wfull.at[q, ch], ag_p.at[k, ch], ag_recv.at[q, ch], seq=partner
        )

    def w_arrived(q, ch):
        remote(
            wfull.at[q, ch], wfull.at[q, ch], ag_p.at[0, 0], ag_recv.at[q, ch], seq=partner
        ).wait_recv()

    for ch in range(2):

        @pl.when(z < Z - 1)
        def _():
            w_right(z, ch, True).start()

        @pl.when(z > 0)
        def _():
            w_left(z, ch, True).start()

        w_swap(z, ch, True).start()

    def g_own(sub, hf):
        return g_ref.at[:, pl.ds(sub * Wr + hf * half, half)]

    def g_local(sub, hf):
        return pltpu.make_async_copy(
            g_own(sub, hf), gfull.at[h * nsub + sub, hf], loc.at[sub, hf]
        )

    for sub in range(nsub):
        for hf in range(2):
            g_local(sub, hf).start()

    def g_to(j, sub, hf):
        q = h * nsub + sub
        return remote(
            g_own(sub, hf), gfull.at[q, hf], g_send.at[j, sub, hf], g_recv.at[q, hf], head=h ^ j
        )

    def g_relay(j, frm, sub, hf):
        q = (h ^ frm) * nsub + sub
        return remote(
            gfull.at[q, hf], gfull.at[q, hf], g_send.at[3, sub, hf], g_recv.at[q, hf], head=h ^ j
        )

    def g_arrived(j, sub, hf):
        q = (h ^ j) * nsub + sub
        remote(
            gfull.at[q, hf], gfull.at[q, hf], g_send.at[j, sub, hf], g_recv.at[q, hf], head=h ^ j
        ).wait_recv()

    subs = range(nsub)
    if H == 4:
        for sub in subs:
            g_to(1, sub, 0).start()
            g_to(2, sub, 1).start()
    else:
        for j in others:
            for sub in subs:
                for hf in range(2):
                    g_to(j, sub, hf).start()

    tiles = T // TILE_ROWS

    def fetch(t, slot):
        rows = pl.ds(t * TILE_ROWS, TILE_ROWS)
        return (
            pltpu.make_async_copy(y_ref.at[rows], ybuf.at[slot], in_sem.at[0, slot]),
            pltpu.make_async_copy(z_ref.at[rows], zbuf.at[slot], in_sem.at[1, slot]),
        )

    def stream(body):
        for copy in fetch(0, 0):
            copy.start()

        @pl.loop(0, tiles)
        def _(t):
            slot = t % 2

            @pl.when(t + 1 < tiles)
            def _():
                for copy in fetch(t + 1, 1 - slot):
                    copy.start()

            for copy in fetch(t, slot):
                copy.wait()
            body(t, slot)

    def square_tile(t, slot):
        @pl.loop(0, TILE_ROWS // ROWS)
        def _(r):
            rows = pl.ds(r * ROWS, ROWS)
            at = pl.ds(t * TILE_ROWS + r * ROWS, ROWS)
            gv = zbuf[slot, rows, :].astype(F32)
            gated = ybuf[slot, rows, :].astype(F32) * (gv * jax.nn.sigmoid(gv))
            acc[at, :] = gated
            sqp[at, :] = lane_sum(gated * gated)

    stream(square_tile)

    def share(buf, send, recv):
        buf[h] = jnp.broadcast_to(jnp.sum(sqp[...].T, axis=0, keepdims=True), (8, T))
        for j in others:
            remote(buf.at[h], buf.at[h], send.at[j], recv.at[h], head=h ^ j).start()

    def shared(buf, send, recv):
        for j in others:
            remote(buf.at[h ^ j], buf.at[h ^ j], send.at[j], recv.at[h ^ j], head=h ^ j).wait_recv()
        total = buf[0, 0:1, :]
        for j in others:
            total = total + buf[j, 0:1, :]
        for j in others:
            remote(buf.at[h], buf.at[h], send.at[j], recv.at[h], head=h ^ j).wait_send()
        return total

    share(sqx, sq_send, sq_recv)

    if H == 4:
        for sub in subs:
            g_arrived(1, sub, 0)
            g_relay(2, 1, sub, 0).start()
        for sub in subs:
            g_arrived(2, sub, 1)
            g_relay(1, 2, sub, 1).start()
        for sub in subs:
            g_to(1, sub, 1).start()
            g_to(2, sub, 0).start()

    inv_row = lax.rsqrt(shared(sqx, sq_send, sq_recv) / DI + epsilon)
    invc[...] = jnp.broadcast_to(inv_row, (128, T)).T

    @pl.loop(0, T // ROWS)
    def _(r):
        at = pl.ds(r * ROWS, ROWS)
        nbuf[at, :] = (acc[at, :] * invc[at, 0:1] * nw_ref[...]).astype(BF16)

    for sub in subs:
        for hf in range(2):
            g_local(sub, hf).wait()
    tri = (
        lax.broadcasted_iota(jnp.int32, (CHUNK, CHUNK), 0)
        <= lax.broadcasted_iota(jnp.int32, (CHUNK, CHUNK), 1)
    ).astype(F32)
    cum_row[...] = jnp.zeros_like(cum_row)
    for q in range(chunks):
        cols = slice(q * CHUNK, (q + 1) * CHUNK)
        cum_row[0:HL, cols] = jnp.dot(
            ld_ref[:, cols], tri, precision=lax.Precision.HIGHEST, preferred_element_type=F32
        )
    cum_col[...] = cum_row[...].T
    spread[...] = (
        lax.broadcasted_iota(jnp.int32, (128, C), 0)
        == lax.broadcasted_iota(jnp.int32, (128, C), 1) // HD
    ).astype(BF16)

    steps_all = [(src, dst, q) for src, dst in ((si_ref, b_ref), (so_ref, c_ref)) for q in range(chunks)]

    def raw_copy(n):
        src, _, q = steps_all[n]
        return pltpu.make_async_copy(
            src.at[pl.ds(q * CHUNK, CHUNK)], raw.at[n % 2], in_sem.at[0, n % 2]
        )

    raw_copy(0).start()
    for n, (_, dst, q) in enumerate(steps_all):
        if n + 1 < len(steps_all):
            raw_copy(n + 1).start()
        raw_copy(n).wait()
        cfc[0 : CHUNK * GROUPS, :] = raw[n % 2].astype(F32).reshape(CHUNK * GROUPS, NS)
        for g in range(NG):
            dst[g, q * CHUNK : (q + 1) * CHUNK, :] = cfc[
                pl.ds(first_group + g, CHUNK, stride=GROUPS), :
            ].astype(BF16)

    def widen(x, g):
        high = x.astype(BF16)
        low = (x - high.astype(F32)).astype(BF16)
        onto = spread[0 : x.shape[1], g * GW : (g + 1) * GW]
        return jnp.dot(high, onto, preferred_element_type=F32) + jnp.dot(
            low, onto, preferred_element_type=F32
        )

    def last_of(q):
        return cum_col[pl.ds(q * CHUNK + CHUNK - 1, 1), :]

    def pair_copy(k, cx, d, ch):
        return remote(
            pst.at[d, ch], pair.at[k, cx], pair_send.at[d, ch], pair_recv.at[k, cx], seq=partner
        )

    def rs_prep(k, cx, d, ch, slot):
        gt[0:half, :] = gfull[2 * k + 1 - c, cx].T
        gt[half:Wr, :] = gfull[2 * k + c, cx].T

        @pl.loop(0, C // TN)
        def _(t):
            cols = pl.ds(pl.multiple_of(t * TN, TN), TN)
            part = jnp.dot(gt[...], nbuf[:, cols], preferred_element_type=F32)
            pst[d, ch, :, cols] = part[:half].astype(BF16)
            ownp[slot, :, cols] = part[half:]

        pair_copy(k, cx, d, ch).start()

    def chain_right(k, cx):
        return remote(
            chain.at[k, cx], chain.at[k, cx], ch_send.at[k, cx], ch_recv.at[k, cx], seq=s + 2
        )

    def chain_left(k, cx):
        to = jnp.where(k == z - 1, Z, k)
        return remote(
            chain.at[k, cx], chain.at[to, cx], ch_send.at[k, cx], ch_recv.at[to, cx], seq=s - 2
        )

    def late_left(k, cx, n):
        rows = pl.ds(n * (half // 2), half // 2)
        if n:
            send, recv = late_sem.at[0], late_sem.at[1]
        else:
            send, recv = ch_send.at[k, cx], ch_recv.at[Z, cx]
        return remote(chain.at[k, cx, rows], chain.at[Z, cx, rows], send, recv, seq=s - 2)

    def late_arrived(cx, n):
        rows = pl.ds(n * (half // 2), half // 2)
        recv = late_sem.at[1] if n else ch_recv.at[Z, cx]
        remote(chain.at[Z, cx, rows], chain.at[Z, cx, rows], ch_send.at[0, 0], recv, seq=partner).wait_recv()

    def chain_arrived(k, cx):
        remote(
            chain.at[k, cx], chain.at[k, cx], ch_send.at[0, 0], ch_recv.at[k, cx], seq=partner
        ).wait_recv()

    def rs_sum(k, cx, d, ch, chained):
        pair_copy(k, cx, d, ch).wait_recv()

        @pl.when(chained)
        def _():
            chain_arrived(k, cx)

            @pl.loop(0, half // ROWS)
            def _(r):
                at = pl.ds(r * ROWS, ROWS)
                chain[k, cx, at, :] = (
                    ownp[d, at, :] + pair[k, cx, at, :].astype(F32) + chain[k, cx, at, :].astype(F32)
                ).astype(BF16)

        @pl.when(jnp.logical_not(chained))
        def _():
            @pl.loop(0, half // ROWS)
            def _(r):
                at = pl.ds(r * ROWS, ROWS)
                chain[k, cx, at, :] = (ownp[d, at, :] + pair[k, cx, at, :].astype(F32)).astype(BF16)

    def half_of(k, ch):
        if H != 4:
            return ch
        return jnp.where((2 * k * Wr // F) ^ h == 2, 1 - ch, ch)

    near = jnp.minimum(z, zm)

    def plane_of(p):
        d = (p + 1) // 2
        close = jnp.where(p % 2 == 1, z - d, z + d)
        far = jnp.where(z < zm, z + (p - near), z - (p - near))
        return jnp.where(p <= 2 * near, close, far)

    def w_load(src, par, ch):
        return pltpu.make_async_copy(
            src, wbuf.at[par, ch, pl.ds(0, half)], wsem.at[par, ch]
        )

    def project(p, first, parts=(0, 1)):
        k = plane_of(p)
        for ch in parts:
            w_arrived(2 * k + 1 - c, ch)
        for par in range(2):
            mine = jnp.logical_and(k == z, c == par)
            for ch in parts:

                @pl.when(mine)
                def _():
                    w_load(w_ref.at[pl.ds(ch * half, half)], par, ch).start()

                @pl.when(jnp.logical_not(mine))
                def _():
                    w_load(wfull.at[2 * k + par, ch], par, ch).start()

        for par in range(2):
            for ch in parts:
                w_load(wfull.at[2 * k + par, ch], par, ch).wait()

        @pl.loop(0, C // TN)
        def _(t):
            cols = pl.ds(pl.multiple_of(t * TN, TN), TN)
            total = None if first else acc[:, cols]
            for par in range(2):
                for ch in parts:
                    part = jnp.dot(
                        gfull[2 * k + par, ch],
                        wbuf[par, ch, 0:half, cols],
                        preferred_element_type=F32,
                    )
                    total = part if total is None else total + part
            acc[:, cols] = total

    def planes_at(slot):
        go_right = jnp.logical_and(slot > z, z < Z - 1)
        go_left = jnp.logical_and(slot > zm, z > 0)
        return go_right, go_left, Z + z - slot, slot - Z + z

    def prep_at(i):
        slot = i // 2
        ch = i % 2
        go_right, go_left, kr, kl = planes_at(slot)

        @pl.when(go_right)
        def _():
            @pl.when(slot - 1 > z)
            def _():
                pair_copy(kr, 0, 0, ch).wait_send()

            rs_prep(kr, half_of(kr, ch), 0, ch, 0)

        @pl.when(go_left)
        def _():
            @pl.when(slot - 1 > zm)
            def _():
                pair_copy(kl, 0, 1, ch).wait_send()

            rs_prep(kl, half_of(kl, ch), 1, ch, 1)

    def block_of(k):
        return 2 * k * Wr // F

    cross_first = jnp.logical_or(
        jnp.logical_and(z == 0, block_of(Z - 1) ^ h == 3),
        jnp.logical_and(z == Z - 1, block_of(0) ^ h == 3),
    )

    def cross_arrived():
        for sub in subs:
            for hf in range(2):
                g_arrived(3, sub, hf)

    @pl.loop(2, 2 * Z)
    def _(i):
        slot = i // 2
        ch = i % 2

        @pl.when(z - slot >= 0)
        def _():
            k = z - slot
            w_arrived(2 * k + c, ch)

            @pl.when(z < Z - 1)
            def _():
                w_right(k, ch).start()

            w_swap(k, ch).start()

        @pl.when(z + slot <= Z - 1)
        def _():
            k = z + slot
            w_arrived(2 * k + c, ch)

            @pl.when(z > 0)
            def _():
                w_left(k, ch).start()

            w_swap(k, ch).start()

        if H == 4:

            @pl.when(jnp.logical_and(i == 2, cross_first))
            def _():
                cross_arrived()

            @pl.when(i == 3)
            def _():
                for sub in subs:
                    g_arrived(1, sub, 1)
                    g_arrived(2, sub, 0)

        else:

            @pl.when(i == 2)
            def _():
                for j in others:
                    for sub in subs:
                        for hf in range(2):
                            g_arrived(j, sub, hf)

        @pl.when(i <= 3)
        def _():
            prep_at(i)

        go_right, go_left, kr, kl = planes_at(slot)

        @pl.when(go_right)
        def _():
            cx = half_of(kr, ch)
            rs_sum(kr, cx, 0, ch, z > 0)
            chain_right(kr, cx).start()

        @pl.when(go_left)
        def _():
            cx = half_of(kl, ch)
            rs_sum(kl, cx, 1, ch, z < Z - 1)
            late = jnp.logical_and(slot == Z - 1, ch == 1)

            @pl.when(late)
            def _():
                late_left(kl, cx, 0).start()

            @pl.when(jnp.logical_not(late))
            def _():
                chain_left(kl, cx).start()

        if H == 4:

            @pl.when(jnp.logical_and(i == 2, jnp.logical_not(cross_first)))
            def _():
                cross_arrived()

        @pl.when(jnp.logical_and(i >= 3, i + 1 < 2 * Z))
        def _():
            prep_at(i + 1)

        @pl.when(i == 3)
        def _():
            project(0, True)

        lo = jnp.where(i == 4, 1, jnp.where(i == 5, 2, slot))
        one = jnp.logical_or(
            jnp.logical_or(i == 4, i == 5), jnp.logical_and(slot >= 3, ch == 1)
        )
        hi = jnp.where(one, jnp.minimum(lo + 1, Z - 1), lo)

        @pl.loop(lo, hi)
        def _(p):
            project(p, False)

        @pl.when(i == 2 * Z - 2)
        def _():
            project(Z - 1, False, (0,))

    project(Z - 1, False, (1,))

    @pl.loop(0, T // ROWS)
    def _(r):
        at = pl.ds(r * ROWS, ROWS)
        sqp[at, :] = lane_sum(acc[at, :] * nbuf[at, :].astype(F32))

    share(wgx, wg_send, wg_recv)
    weighted = shared(wgx, wg_send, wg_recv) / DI
    cfc[...] = jnp.broadcast_to(weighted, (128, T)).T * invc[...] * invc[...]

    def put(t, slot):
        rows = pl.ds(t * TILE_ROWS, TILE_ROWS)
        return pltpu.make_async_copy(obuf.at[slot], gate_out.at[rows], out_sem.at[0, slot])

    quarter = tiles // 4
    per_quarter = T // 4 // CHUNK

    def grad_at(q):
        rows = pl.ds(pl.multiple_of((q % per_quarter) * CHUNK, CHUNK), CHUNK)
        return q // (2 * per_quarter), (q // per_quarter) % 2, rows

    def grad_tile(t, slot):
        @pl.when(t >= 2)
        def _():
            put(t - 2, slot).wait()

        @pl.loop(0, TILE_ROWS // ROWS)
        def _(r):
            rows = pl.ds(r * ROWS, ROWS)
            at = pl.ds(t * TILE_ROWS + r * ROWS, ROWS)
            gv = zbuf[slot, rows, :].astype(F32)
            values = ybuf[slot, rows, :].astype(F32)
            sig = jax.nn.sigmoid(gv)
            silu = gv * sig
            gg = invc[at, 0:1] * nw_ref[...] * acc[at, :] - values * silu * cfc[at, 0:1]
            obuf[slot, rows, :] = (gg * values * sig * (1.0 + gv * (1.0 - sig))).astype(BF16)
            here = pl.ds((t % quarter) * TILE_ROWS + r * ROWS, ROWS)
            wbuf[t // (2 * quarter), (t // quarter) % 2, here, :] = (gg * silu).astype(BF16)

        put(t, slot).start()

    stream(grad_tile)
    for t in (tiles - 2, tiles - 1):
        put(t, t % 2).wait()

    pads = jnp.zeros((128 - HL, T), F32)
    cfc[...] = jnp.concatenate([ts_ref[...], pads], axis=0).T
    per = 2 * half // CHUNK

    def inside(q):
        plane = lax.rem(z + 1 + q // per, Z)
        r = q % per
        rows = half // CHUNK
        return plane, r // rows, pl.ds(pl.multiple_of((r % rows) * CHUNK, CHUNK), CHUNK)

    run[...] = jnp.zeros_like(run)

    @pl.loop(0, chunks, init_carry=jnp.zeros((1, 128), F32))
    def tail(step, later):
        q = chunks - 1 - step
        at = pl.ds(pl.multiple_of(q * CHUNK, CHUNK), CHUNK)
        total = last_of(q)
        sqp[at, :] = total - cum_col[at, :] + later
        grow = jnp.exp(cum_col[at, :])
        keep = jnp.exp(jnp.broadcast_to(total, (8, 128)))
        plane, hf, rows = inside(q)
        wa, wb, wr = grad_at(q)
        for g in range(NG):
            cols = slice(g * GW, (g + 1) * GW)
            scaled = (widen(grow, g) * wbuf[wa, wb, wr, cols].astype(F32)).astype(BF16)
            state = jnp.dot(c_ref[g, at, :].T, scaled, preferred_element_type=F32)
            pair[plane, hf, rows, cols] = run[:, cols].astype(BF16)
            run[:, cols] = state + widen(keep, g)[0:1, :] * run[:, cols]
        return later + total

    summ[c] = run[...].astype(BF16)
    keep_all = jnp.exp(jnp.broadcast_to(tail, (8, 128)))
    for g in range(NG):
        decay[c, :, g * GW : (g + 1) * GW] = widen(keep_all, g)

    def swaps():
        return (
            remote(summ.at[c], summ.at[c], swap_send.at[0], swap_recv.at[0], seq=partner),
            remote(decay.at[c], decay.at[c], swap_send.at[1], swap_recv.at[1], seq=partner),
        )

    for copy in swaps():
        copy.start()

    def state_left(part):
        rows = pl.ds(part * (NS // PARTS), NS // PARTS)
        return remote(
            vbuf.at[rows], rbuf.at[c, rows], st_send.at[part], st_recv.at[part], seq=s - 2
        )

    def state_swap(part):
        rows = pl.ds(part * (NS // PARTS), NS // PARTS)
        return remote(
            rbuf.at[c, rows], rbuf.at[c, rows], half_send.at[part], half_recv.at[part], seq=partner
        )

    mine_cols = pl.ds(pl.multiple_of(c * CH, CH), CH)

    def state_step(part):
        rows = pl.ds(part * (NS // PARTS), NS // PARTS)

        @pl.when(z < Z - 1)
        def _():
            state_left(part).wait_recv()
            state_swap(part).start()

        @pl.when(z > 0)
        def _():
            first_keep = decay[0, 0:1, mine_cols]
            here = summ[0, rows, mine_cols].astype(F32) + first_keep * summ[
                1, rows, mine_cols
            ].astype(F32)

            @pl.when(z < Z - 1)
            def _():
                vbuf[rows, :] = (
                    here
                    + first_keep * decay[1, 0:1, mine_cols] * rbuf[c, rows, :].astype(F32)
                ).astype(BF16)

            @pl.when(z == Z - 1)
            def _():
                vbuf[rows, :] = here.astype(BF16)

            state_left(part).start()

    upper = lax.broadcasted_iota(jnp.int32, (CHUNK, CHUNK), 1) >= lax.broadcasted_iota(
        jnp.int32, (CHUNK, CHUNK), 0
    )
    lane = lax.broadcasted_iota(jnp.int32, (CHUNK, 2 * HD), 1)

    @pl.loop(0, chunks)
    def _(q):
        @pl.when(q == 0)
        def _():
            for copy in swaps():
                copy.wait_recv()

        for part in range(PARTS):

            @pl.when(q == jnp.where(zm == 0, 0, jnp.minimum(2 * zm + part, chunks - 1)))
            def _():
                state_step(part)

        at = pl.ds(pl.multiple_of(q * CHUNK, CHUNK), CHUNK)
        plane, hf, rows = inside(q)
        wa, wb, wr = grad_at(q)
        cum = cum_col[at, :]
        fade = jnp.exp(last_of(q) - cum)
        steps = cfc[at, :]
        skips = jnp.broadcast_to(skip_ref[...], (8, HL))
        for g in range(NG):
            b = b_ref[g, at, :]
            scores = lax.dot_general(
                b, c_ref[g, at, :], (((1,), (1,)), ((), ())), preferred_element_type=F32
            )
            scores = jnp.where(upper, scores, 0.0)
            cols = slice(g * GW, (g + 1) * GW)
            acc[at, cols] = widen(fade, g) * jnp.dot(
                b, pair[plane, hf, rows, cols], preferred_element_type=F32
            )
            for j in range(HPG // 2):
                weights = []
                for head in (g * HPG + 2 * j, g * HPG + 2 * j + 1):
                    gap = cum_row[head : head + 1, at] - cum[:, head : head + 1]
                    weights.append((scores * jnp.exp(jnp.minimum(gap, 0.0))).astype(BF16))
                span = slice(g * GW + 2 * j * HD, g * GW + 2 * (j + 1) * HD)
                both = wbuf[wa, wb, wr, span]
                zero = jnp.zeros_like(both)
                stacked = jnp.concatenate(
                    [jnp.where(lane < HD, both, zero), jnp.where(lane < HD, zero, both)], axis=0
                )
                acc[at, span] = acc[at, span] + jnp.dot(
                    jnp.concatenate(weights, axis=1), stacked, preferred_element_type=F32
                )
            acc[at, cols] = widen(steps, g) * acc[at, cols] + widen(skips, g)[0:1, :] * wbuf[
                wa, wb, wr, cols
            ].astype(F32)

    @pl.when(z > 0)
    def _():
        late_left(z - 1, half_of(z - 1, 1), 1).start()

    for ch in range(2):

        @pl.when(Z - 1 > z)
        def _():
            pair_copy(z, ch, 0, ch).wait_send()

        rs_prep(z, ch, 0, ch, ch)

    @pl.when(z < Z - 1)
    def _():
        for part in range(PARTS):
            rows = pl.ds(part * (NS // PARTS), NS // PARTS)
            remote(
                rbuf.at[1 - c, rows],
                rbuf.at[1 - c, rows],
                half_send.at[part],
                half_recv.at[part],
                seq=partner,
            ).wait_recv()

    @pl.when(z == Z - 1)
    def _():
        rbuf[...] = jnp.zeros_like(rbuf)

    for side in range(2):
        cols = slice(side * CH, (side + 1) * CH)
        later = rbuf[side].astype(F32)

        @pl.when(c == 1)
        def _():
            arrived[:, cols] = later.astype(BF16)

        @pl.when(c == 0)
        def _():
            arrived[:, cols] = (
                summ[1, :, cols].astype(F32) + decay[1, 0:1, cols] * later
            ).astype(BF16)

    def put_x(t, slot):
        rows = pl.ds(t * TILE_ROWS, TILE_ROWS)
        return pltpu.make_async_copy(ybuf.at[slot], gx_out.at[rows], out_sem.at[1, slot])

    @pl.loop(0, tiles)
    def _(t):
        slot = t % 2
        at = pl.ds(pl.multiple_of(t * TILE_ROWS, TILE_ROWS), TILE_ROWS)

        @pl.when(t >= 2)
        def _():
            put_x(t - 2, slot).wait()

        factor = cfc[at, :] * jnp.exp(sqp[at, :])
        for g in range(NG):
            cols = slice(g * GW, (g + 1) * GW)
            ybuf[slot, :, cols] = (
                acc[at, cols]
                + widen(factor, g)
                * jnp.dot(b_ref[g, at, :], arrived[:, cols], preferred_element_type=F32)
            ).astype(BF16)
        put_x(t, slot).start()

    scale = 1.0 / math.sqrt(T * S)

    def gow_copy(ch):
        rows = pl.ds(ch * half, half)
        return pltpu.make_async_copy(ownp.at[ch], gow_out.at[rows], out_sem.at[0, ch])

    for ch in range(2):
        pair_copy(z, ch, 0, ch).wait_recv()

        @pl.loop(0, half // ROWS)
        def _(r):
            at = pl.ds(r * ROWS, ROWS)
            ownp[ch, at, :] = ownp[ch, at, :] + pair[z, ch, at, :].astype(F32)

    for first, from_slot in ((0, z), (Z - 1, Z)):
        for step in range(2):

            @pl.when(z != first)
            def _():
                ch = half_of(z, step)
                if first == Z - 1 and step == 1:
                    late_arrived(ch, 0)
                    late_arrived(ch, 1)
                else:
                    chain_arrived(from_slot, ch)

                @pl.loop(0, half // ROWS)
                def _(r):
                    at = pl.ds(r * ROWS, ROWS)
                    ownp[ch, at, :] = ownp[ch, at, :] + chain[from_slot, ch, at, :].astype(F32)

    for ch in range(2):

        @pl.loop(0, half // ROWS)
        def _(r):
            at = pl.ds(r * ROWS, ROWS)
            ownp[ch, at, :] = ownp[ch, at, :] * scale

        gow_copy(ch).start()

    for t in (tiles - 2, tiles - 1):
        put_x(t, t % 2).wait()

    for copy in swaps():
        copy.wait_send()
    for part in range(PARTS):

        @pl.when(z < Z - 1)
        def _():
            state_swap(part).wait_send()

        @pl.when(z > 0)
        def _():
            state_left(part).wait_send()

    for ch in range(2):
        pair_copy(z, ch, 0, ch).wait_send()

        @pl.when(z > 0)
        def _():
            pair_copy(z, ch, 1, ch).wait_send()

        @pl.loop(0, Z)
        def _(k):
            w_swap(k, ch).wait_send()

            @pl.when(jnp.logical_and(k <= z, z < Z - 1))
            def _():
                w_right(k, ch).wait_send()

            @pl.when(jnp.logical_and(k >= z, z > 0))
            def _():
                w_left(k, ch).wait_send()

            @pl.when(k > z)
            def _():
                chain_right(k, ch).wait_send()

            late = jnp.logical_and(k == z - 1, half_of(k, 1) == ch)

            @pl.when(jnp.logical_and(k < z, late))
            def _():
                late_left(k, ch, 0).wait_send()
                late_left(k, ch, 1).wait_send()

            @pl.when(jnp.logical_and(k < z, jnp.logical_not(late)))
            def _():
                chain_left(k, ch).wait_send()

    for sub in subs:
        if H == 4:
            g_relay(2, 1, sub, 0).wait_send()
            g_relay(1, 2, sub, 1).wait_send()
        for j in others if H != 4 else (1, 2):
            for hf in range(2):
                g_to(j, sub, hf).wait_send()
    for ch in range(2):
        gow_copy(ch).wait()


def mixer(
    grad_output,
    out_weight,
    ssd_out,
    gate,
    norm_weight,
    time_step,
    log_decay,
    state_in,
    state_out,
    skip,
):
    S, H = lax.axis_size("seq"), lax.axis_size("head")
    T, F = grad_output.shape
    Wr, C = out_weight.shape
    Z = S // 2
    half = Wr // 2
    nsub = F // Wr
    heads_here = time_step.shape[0]
    groups_here = max(1, heads_here * GROUPS // HEADS)
    NS = state_in.shape[2]
    hbm = pl.BlockSpec(memory_space=pl.ANY)
    vmem = pl.BlockSpec(memory_space=pltpu.VMEM)
    dma = pltpu.SemaphoreType.DMA
    flops = 4 * T * F * H * C
    outs = pl.pallas_call(
        functools.partial(mixer_kernel, (S, H, T, F, Wr, C)),
        out_shape=(
            jax.ShapeDtypeStruct((T, C), BF16),
            jax.ShapeDtypeStruct((T, C), BF16),
            jax.ShapeDtypeStruct((Wr, C), F32),
            jax.ShapeDtypeStruct((S, 2, half, C), BF16),
        ),
        in_specs=[hbm] * 4 + [vmem] * 3 + [hbm] * 2 + [vmem],
        out_specs=(hbm,) * 4,
        scratch_shapes=[
            pltpu.VMEM((S, 2, T, half), BF16),
            pltpu.VMEM((T, C), BF16),
            pltpu.VMEM((T, C), F32),
            pltpu.VMEM((Z, 2, half, C), BF16),
            pltpu.VMEM((Z + 1, 2, half, C), BF16),
            pltpu.VMEM((2, 2, half, C), BF16),
            pltpu.VMEM((2, half, C), F32),
            pltpu.VMEM((Wr, T), BF16),
            pltpu.VMEM((2, 2, max(half, T // 4), C), BF16),
            pltpu.VMEM((2, TILE_ROWS, C), BF16),
            pltpu.VMEM((2, TILE_ROWS, C), BF16),
            pltpu.VMEM((2, TILE_ROWS, C), BF16),
            pltpu.VMEM((T, 128), F32),
            pltpu.VMEM((H, 8, T), F32),
            pltpu.VMEM((H, 8, T), F32),
            pltpu.VMEM((T, 128), F32),
            pltpu.VMEM((T, 128), F32),
            pltpu.VMEM((128, T), F32),
            pltpu.VMEM((T, 128), F32),
            pltpu.VMEM((128, C), BF16),
            pltpu.VMEM((NS, C), F32),
            pltpu.VMEM((2, NS, C), BF16),
            pltpu.VMEM((2, 8, C), F32),
            pltpu.VMEM((2, NS, C // 2), BF16),
            pltpu.VMEM((NS, C // 2), BF16),
            pltpu.VMEM((NS, C), BF16),
            pltpu.VMEM((2, CHUNK, GROUPS, NS), BF16),
            pltpu.VMEM((groups_here, T, NS), BF16),
            pltpu.VMEM((groups_here, T, NS), BF16),
            dma((S, 2)),
            dma((Z, 2)),
            dma((Z, 2)),
            dma((Z, 2)),
            dma((S, 2)),
            dma((H, nsub, 2)),
            dma((H,)),
            dma((H,)),
            dma((H,)),
            dma((H,)),
            dma((Z, 2)),
            dma((2, 2)),
            dma((Z + 1, 2)),
            dma((Z, 2)),
            dma((nsub, 2)),
            dma((2, 2)),
            dma((2, 2)),
            dma((2, 2)),
            dma((2,)),
            dma((2,)),
            dma((4,)),
            dma((4,)),
            dma((4,)),
            dma((4,)),
            dma((2,)),
        ],
        compiler_params=pltpu.CompilerParams(
            collective_id=0, has_side_effects=True, vmem_limit_bytes=67043328
        ),
        cost_estimate=pl.CostEstimate(flops=flops, bytes_accessed=64 << 20, transcendentals=0),
        name="mixer",
    )(
        grad_output,
        out_weight,
        ssd_out,
        gate,
        norm_weight.reshape(1, C),
        time_step,
        log_decay,
        state_in,
        state_out,
        skip.reshape(1, heads_here),
    )
    grad_gate, grad_x, grad_out_weight, _ = outs
    return grad_x, grad_gate, grad_out_weight


def solution(mesh):
    return jax.shard_map(
        mixer,
        mesh=mesh,
        in_specs=(
            P("seq", "head"),
            P("seq", "head"),
            P("seq", "head"),
            P("seq", "head"),
            P("head"),
            P("head", "seq"),
            P("head", "seq"),
            P("seq", None, None),
            P("seq", None, None),
            P("head"),
        ),
        out_specs=(P("seq", "head"), P("seq", "head"), P("seq", "head")),
        check_vma=False,
    )
```

```python
import functools
import math

import jax
import jax.numpy as jnp
from jax import lax
from jax.experimental import pallas as pl
from jax.experimental.pallas import tpu as pltpu
from jax.sharding import PartitionSpec as P

HEADS = 128
GROUPS = 8
BLOCK_LEN = 256
MESH = pl.DeviceIdType.MESH
F32 = jnp.float32
BF16 = jnp.bfloat16
ROWS = 16
TILE_ROWS = 64
CHUNK = 128


epsilon = 1e-05


def remote(src, dst, send_sem, recv_sem, **device):
    return pltpu.make_async_remote_copy(
        src_ref=src,
        dst_ref=dst,
        send_sem=send_sem,
        recv_sem=recv_sem,
        device_id=device,
        device_id_type=MESH,
    )


def lane_sum(x):
    total = x[:, 0:128]
    for j in range(1, x.shape[1] // 128):
        total = total + x[:, j * 128 : (j + 1) * 128]
    return total


def mixer_kernel(
    dims,
    g_ref,
    w_ref,
    y_ref,
    z_ref,
    nw_ref,
    ts_ref,
    ld_ref,
    si_ref,
    so_ref,
    skip_ref,
    gate_out,
    gx_out,
    gow_out,
    wfull,
    gfull,
    nbuf,
    acc,
    pair,
    chain,
    pst,
    ownp,
    gt,
    wbuf,
    ybuf,
    zbuf,
    obuf,
    sqp,
    sqx,
    wgx,
    invc,
    cfc,
    cum_row,
    cum_col,
    spread,
    run,
    summ,
    decay,
    rbuf,
    vbuf,
    arrived,
    raw,
    b_ref,
    c_ref,
    ag_recv,
    ag_r,
    ag_l,
    ag_p,
    g_recv,
    g_send,
    sq_recv,
    sq_send,
    wg_recv,
    wg_send,
    pair_recv,
    pair_send,
    ch_recv,
    ch_send,
    loc,
    wsem,
    in_sem,
    out_sem,
    swap_recv,
    swap_send,
    st_recv,
    st_send,
    half_recv,
    half_send,
    late_sem,
):
    S, H, T, F, Wr, C = dims
    Z = S // 2
    half = Wr // 2
    nsub = F // Wr
    DI = C * H
    TN = min(256, C)
    HL = ld_ref.shape[0]
    HD = C // HL
    GW = min(C, (HEADS // GROUPS) * HD)
    NG = C // GW
    HPG = GW // HD
    NS = si_ref.shape[2]
    CH = C // 2
    chunks = T // CHUNK
    PARTS = 4
    s = lax.axis_index("seq")
    h = lax.axis_index("head")
    z = s // 2
    c = s % 2
    zm = Z - 1 - z
    first_group = h * HL // (HEADS // GROUPS)
    partner = s + 1 - 2 * c
    others = range(1, H)

    barrier = pltpu.get_barrier_semaphore()
    pl.semaphore_signal(barrier, inc=1, device_id={"seq": partner}, device_id_type=MESH)
    for j in others:
        pl.semaphore_signal(barrier, inc=1, device_id={"head": h ^ j}, device_id_type=MESH)

    @pl.when(z > 0)
    def _():
        pl.semaphore_signal(barrier, inc=1, device_id={"seq": s - 2}, device_id_type=MESH)

    @pl.when(z < Z - 1)
    def _():
        pl.semaphore_signal(barrier, inc=1, device_id={"seq": s + 2}, device_id_type=MESH)

    peers = H + jnp.where(z > 0, 1, 0) + jnp.where(z < Z - 1, 1, 0)
    pl.semaphore_wait(barrier, peers)

    def w_src(k, ch, own):
        return w_ref.at[pl.ds(ch * half, half)] if own else wfull.at[2 * k + c, ch]

    def w_right(k, ch, own=False):
        q = 2 * k + c
        return remote(
            w_src(k, ch, own), wfull.at[q, ch], ag_r.at[k, ch], ag_recv.at[q, ch], seq=s + 2
        )

    def w_left(k, ch, own=False):
        q = 2 * k + c
        return remote(
            w_src(k, ch, own), wfull.at[q, ch], ag_l.at[k, ch], ag_recv.at[q, ch], seq=s - 2
        )

    def w_swap(k, ch, own=False):
        q = 2 * k + c
        return remote(
            w_src(k, ch, own), wfull.at[q, ch], ag_p.at[k, ch], ag_recv.at[q, ch], seq=partner
        )

    def w_arrived(q, ch):
        remote(
            wfull.at[q, ch], wfull.at[q, ch], ag_p.at[0, 0], ag_recv.at[q, ch], seq=partner
        ).wait_recv()

    for ch in range(2):

        @pl.when(z < Z - 1)
        def _():
            w_right(z, ch, True).start()

        @pl.when(z > 0)
        def _():
            w_left(z, ch, True).start()

        w_swap(z, ch, True).start()

    def g_own(sub, hf):
        return g_ref.at[:, pl.ds(sub * Wr + hf * half, half)]

    def g_local(sub, hf):
        return pltpu.make_async_copy(
            g_own(sub, hf), gfull.at[h * nsub + sub, hf], loc.at[sub, hf]
        )

    for sub in range(nsub):
        for hf in range(2):
            g_local(sub, hf).start()

    def g_to(j, sub, hf):
        q = h * nsub + sub
        return remote(
            g_own(sub, hf), gfull.at[q, hf], g_send.at[j, sub, hf], g_recv.at[q, hf], head=h ^ j
        )

    def g_relay(j, frm, sub, hf):
        q = (h ^ frm) * nsub + sub
        return remote(
            gfull.at[q, hf], gfull.at[q, hf], g_send.at[3, sub, hf], g_recv.at[q, hf], head=h ^ j
        )

    def g_arrived(j, sub, hf):
        q = (h ^ j) * nsub + sub
        remote(
            gfull.at[q, hf], gfull.at[q, hf], g_send.at[j, sub, hf], g_recv.at[q, hf], head=h ^ j
        ).wait_recv()

    subs = range(nsub)
    if H == 4:
        for sub in subs:
            g_to(1, sub, 0).start()
            g_to(2, sub, 1).start()
    else:
        for j in others:
            for sub in subs:
                for hf in range(2):
                    g_to(j, sub, hf).start()

    tiles = T // TILE_ROWS

    def fetch(t, slot):
        rows = pl.ds(t * TILE_ROWS, TILE_ROWS)
        return (
            pltpu.make_async_copy(y_ref.at[rows], ybuf.at[slot], in_sem.at[0, slot]),
            pltpu.make_async_copy(z_ref.at[rows], zbuf.at[slot], in_sem.at[1, slot]),
        )

    def stream(body):
        for copy in fetch(0, 0):
            copy.start()

        @pl.loop(0, tiles)
        def _(t):
            slot = t % 2

            @pl.when(t + 1 < tiles)
            def _():
                for copy in fetch(t + 1, 1 - slot):
                    copy.start()

            for copy in fetch(t, slot):
                copy.wait()
            body(t, slot)

    def square_tile(t, slot):
        @pl.loop(0, TILE_ROWS // ROWS)
        def _(r):
            rows = pl.ds(r * ROWS, ROWS)
            at = pl.ds(t * TILE_ROWS + r * ROWS, ROWS)
            gv = zbuf[slot, rows, :].astype(F32)
            gated = ybuf[slot, rows, :].astype(F32) * (gv * jax.nn.sigmoid(gv))
            acc[at, :] = gated
            sqp[at, :] = lane_sum(gated * gated)

    stream(square_tile)

    def share(buf, send, recv):
        buf[h] = jnp.broadcast_to(jnp.sum(sqp[...].T, axis=0, keepdims=True), (8, T))
        for j in others:
            remote(buf.at[h], buf.at[h], send.at[j], recv.at[h], head=h ^ j).start()

    def shared(buf, send, recv):
        for j in others:
            remote(buf.at[h ^ j], buf.at[h ^ j], send.at[j], recv.at[h ^ j], head=h ^ j).wait_recv()
        total = buf[0, 0:1, :]
        for j in others:
            total = total + buf[j, 0:1, :]
        for j in others:
            remote(buf.at[h], buf.at[h], send.at[j], recv.at[h], head=h ^ j).wait_send()
        return total

    share(sqx, sq_send, sq_recv)

    if H == 4:
        for sub in subs:
            g_arrived(1, sub, 0)
            g_relay(2, 1, sub, 0).start()
        for sub in subs:
            g_arrived(2, sub, 1)
            g_relay(1, 2, sub, 1).start()
        for sub in subs:
            g_to(1, sub, 1).start()
            g_to(2, sub, 0).start()

    inv_row = lax.rsqrt(shared(sqx, sq_send, sq_recv) / DI + epsilon)
    invc[...] = jnp.broadcast_to(inv_row, (128, T)).T

    @pl.loop(0, T // ROWS)
    def _(r):
        at = pl.ds(r * ROWS, ROWS)
        nbuf[at, :] = (acc[at, :] * invc[at, 0:1] * nw_ref[...]).astype(BF16)

    for sub in subs:
        for hf in range(2):
            g_local(sub, hf).wait()
    tri = (
        lax.broadcasted_iota(jnp.int32, (CHUNK, CHUNK), 0)
        <= lax.broadcasted_iota(jnp.int32, (CHUNK, CHUNK), 1)
    ).astype(F32)
    cum_row[...] = jnp.zeros_like(cum_row)
    for q in range(chunks):
        cols = slice(q * CHUNK, (q + 1) * CHUNK)
        cum_row[0:HL, cols] = jnp.dot(
            ld_ref[:, cols], tri, precision=lax.Precision.HIGHEST, preferred_element_type=F32
        )
    cum_col[...] = cum_row[...].T
    spread[...] = (
        lax.broadcasted_iota(jnp.int32, (128, C), 0)
        == lax.broadcasted_iota(jnp.int32, (128, C), 1) // HD
    ).astype(BF16)

    steps_all = [(src, dst, q) for src, dst in ((si_ref, b_ref), (so_ref, c_ref)) for q in range(chunks)]

    def raw_copy(n):
        src, _, q = steps_all[n]
        return pltpu.make_async_copy(
            src.at[pl.ds(q * CHUNK, CHUNK)], raw.at[n % 2], in_sem.at[0, n % 2]
        )

    raw_copy(0).start()
    for n, (_, dst, q) in enumerate(steps_all):
        if n + 1 < len(steps_all):
            raw_copy(n + 1).start()
        raw_copy(n).wait()
        cfc[0 : CHUNK * GROUPS, :] = raw[n % 2].astype(F32).reshape(CHUNK * GROUPS, NS)
        for g in range(NG):
            dst[g, q * CHUNK : (q + 1) * CHUNK, :] = cfc[
                pl.ds(first_group + g, CHUNK, stride=GROUPS), :
            ].astype(BF16)

    def widen(x, g):
        high = x.astype(BF16)
        low = (x - high.astype(F32)).astype(BF16)
        onto = spread[0 : x.shape[1], g * GW : (g + 1) * GW]
        return jnp.dot(high, onto, preferred_element_type=F32) + jnp.dot(
            low, onto, preferred_element_type=F32
        )

    def last_of(q):
        return cum_col[pl.ds(q * CHUNK + CHUNK - 1, 1), :]

    def pair_copy(k, cx, d, ch):
        return remote(
            pst.at[d, ch], pair.at[k, cx], pair_send.at[d, ch], pair_recv.at[k, cx], seq=partner
        )

    def rs_prep(k, cx, d, ch, slot):
        gt[0:half, :] = gfull[2 * k + 1 - c, cx].T
        gt[half:Wr, :] = gfull[2 * k + c, cx].T

        @pl.loop(0, C // TN)
        def _(t):
            cols = pl.ds(pl.multiple_of(t * TN, TN), TN)
            part = jnp.dot(gt[...], nbuf[:, cols], preferred_element_type=F32)
            pst[d, ch, :, cols] = part[:half].astype(BF16)
            ownp[slot, :, cols] = part[half:]

        pair_copy(k, cx, d, ch).start()

    def chain_right(k, cx):
        return remote(
            chain.at[k, cx], chain.at[k, cx], ch_send.at[k, cx], ch_recv.at[k, cx], seq=s + 2
        )

    def chain_left(k, cx):
        to = jnp.where(k == z - 1, Z, k)
        return remote(
            chain.at[k, cx], chain.at[to, cx], ch_send.at[k, cx], ch_recv.at[to, cx], seq=s - 2
        )

    def late_left(k, cx, n):
        rows = pl.ds(n * (half // 2), half // 2)
        if n:
            send, recv = late_sem.at[0], late_sem.at[1]
        else:
            send, recv = ch_send.at[k, cx], ch_recv.at[Z, cx]
        return remote(chain.at[k, cx, rows], chain.at[Z, cx, rows], send, recv, seq=s - 2)

    def late_arrived(cx, n):
        rows = pl.ds(n * (half // 2), half // 2)
        recv = late_sem.at[1] if n else ch_recv.at[Z, cx]
        remote(chain.at[Z, cx, rows], chain.at[Z, cx, rows], ch_send.at[0, 0], recv, seq=partner).wait_recv()

    def chain_arrived(k, cx):
        remote(
            chain.at[k, cx], chain.at[k, cx], ch_send.at[0, 0], ch_recv.at[k, cx], seq=partner
        ).wait_recv()

    def rs_sum(k, cx, d, ch, chained):
        pair_copy(k, cx, d, ch).wait_recv()

        @pl.when(chained)
        def _():
            chain_arrived(k, cx)

            @pl.loop(0, half // ROWS)
            def _(r):
                at = pl.ds(r * ROWS, ROWS)
                chain[k, cx, at, :] = (
                    ownp[d, at, :] + pair[k, cx, at, :].astype(F32) + chain[k, cx, at, :].astype(F32)
                ).astype(BF16)

        @pl.when(jnp.logical_not(chained))
        def _():
            @pl.loop(0, half // ROWS)
            def _(r):
                at = pl.ds(r * ROWS, ROWS)
                chain[k, cx, at, :] = (ownp[d, at, :] + pair[k, cx, at, :].astype(F32)).astype(BF16)

    def half_of(k, ch):
        if H != 4:
            return ch
        return jnp.where((2 * k * Wr // F) ^ h == 2, 1 - ch, ch)

    near = jnp.minimum(z, zm)

    def plane_of(p):
        d = (p + 1) // 2
        close = jnp.where(p % 2 == 1, z - d, z + d)
        far = jnp.where(z < zm, z + (p - near), z - (p - near))
        return jnp.where(p <= 2 * near, close, far)

    def w_load(src, par, ch):
        return pltpu.make_async_copy(
            src, wbuf.at[par, ch, pl.ds(0, half)], wsem.at[par, ch]
        )

    def project(p, first, parts=(0, 1)):
        k = plane_of(p)
        for ch in parts:
            w_arrived(2 * k + 1 - c, ch)
        for par in range(2):
            mine = jnp.logical_and(k == z, c == par)
            for ch in parts:

                @pl.when(mine)
                def _():
                    w_load(w_ref.at[pl.ds(ch * half, half)], par, ch).start()

                @pl.when(jnp.logical_not(mine))
                def _():
                    w_load(wfull.at[2 * k + par, ch], par, ch).start()

        for par in range(2):
            for ch in parts:
                w_load(wfull.at[2 * k + par, ch], par, ch).wait()

        @pl.loop(0, C // TN)
        def _(t):
            cols = pl.ds(pl.multiple_of(t * TN, TN), TN)
            total = None if first else acc[:, cols]
            for par in range(2):
                for ch in parts:
                    part = jnp.dot(
                        gfull[2 * k + par, ch],
                        wbuf[par, ch, 0:half, cols],
                        preferred_element_type=F32,
                    )
                    total = part if total is None else total + part
            acc[:, cols] = total

    def planes_at(slot):
        go_right = jnp.logical_and(slot > z, z < Z - 1)
        go_left = jnp.logical_and(slot > zm, z > 0)
        return go_right, go_left, Z + z - slot, slot - Z + z

    def prep_at(i):
        slot = i // 2
        ch = i % 2
        go_right, go_left, kr, kl = planes_at(slot)

        @pl.when(go_right)
        def _():
            @pl.when(slot - 1 > z)
            def _():
                pair_copy(kr, 0, 0, ch).wait_send()

            rs_prep(kr, half_of(kr, ch), 0, ch, 0)

        @pl.when(go_left)
        def _():
            @pl.when(slot - 1 > zm)
            def _():
                pair_copy(kl, 0, 1, ch).wait_send()

            rs_prep(kl, half_of(kl, ch), 1, ch, 1)

    def block_of(k):
        return 2 * k * Wr // F

    cross_first = jnp.logical_or(
        jnp.logical_and(z == 0, block_of(Z - 1) ^ h == 3),
        jnp.logical_and(z == Z - 1, block_of(0) ^ h == 3),
    )

    def cross_arrived():
        for sub in subs:
            for hf in range(2):
                g_arrived(3, sub, hf)

    @pl.loop(2, 2 * Z)
    def _(i):
        slot = i // 2
        ch = i % 2

        @pl.when(z - slot >= 0)
        def _():
            k = z - slot
            w_arrived(2 * k + c, ch)

            @pl.when(z < Z - 1)
            def _():
                w_right(k, ch).start()

            w_swap(k, ch).start()

        @pl.when(z + slot <= Z - 1)
        def _():
            k = z + slot
            w_arrived(2 * k + c, ch)

            @pl.when(z > 0)
            def _():
                w_left(k, ch).start()

            w_swap(k, ch).start()

        if H == 4:

            @pl.when(jnp.logical_and(i == 2, cross_first))
            def _():
                cross_arrived()

            @pl.when(i == 3)
            def _():
                for sub in subs:
                    g_arrived(1, sub, 1)
                    g_arrived(2, sub, 0)

        else:

            @pl.when(i == 2)
            def _():
                for j in others:
                    for sub in subs:
                        for hf in range(2):
                            g_arrived(j, sub, hf)

        @pl.when(i <= 3)
        def _():
            prep_at(i)

        go_right, go_left, kr, kl = planes_at(slot)

        @pl.when(go_right)
        def _():
            cx = half_of(kr, ch)
            rs_sum(kr, cx, 0, ch, z > 0)
            chain_right(kr, cx).start()

        @pl.when(go_left)
        def _():
            cx = half_of(kl, ch)
            rs_sum(kl, cx, 1, ch, z < Z - 1)
            late = jnp.logical_and(slot == Z - 1, ch == 1)

            @pl.when(late)
            def _():
                late_left(kl, cx, 0).start()

            @pl.when(jnp.logical_not(late))
            def _():
                chain_left(kl, cx).start()

        if H == 4:

            @pl.when(jnp.logical_and(i == 2, jnp.logical_not(cross_first)))
            def _():
                cross_arrived()

        @pl.when(jnp.logical_and(i >= 3, i + 1 < 2 * Z))
        def _():
            prep_at(i + 1)

        @pl.when(i == 3)
        def _():
            project(0, True)

        lo = jnp.where(i == 4, 1, jnp.where(i == 5, 2, slot))
        one = jnp.logical_or(
            jnp.logical_or(i == 4, i == 5), jnp.logical_and(slot >= 3, ch == 1)
        )
        hi = jnp.where(one, jnp.minimum(lo + 1, Z - 1), lo)

        @pl.loop(lo, hi)
        def _(p):
            project(p, False)

        @pl.when(i == 2 * Z - 2)
        def _():
            project(Z - 1, False, (0,))

    project(Z - 1, False, (1,))

    @pl.loop(0, T // ROWS)
    def _(r):
        at = pl.ds(r * ROWS, ROWS)
        sqp[at, :] = lane_sum(acc[at, :] * nbuf[at, :].astype(F32))

    share(wgx, wg_send, wg_recv)
    weighted = shared(wgx, wg_send, wg_recv) / DI
    cfc[...] = jnp.broadcast_to(weighted, (128, T)).T * invc[...] * invc[...]

    def put(t, slot):
        rows = pl.ds(t * TILE_ROWS, TILE_ROWS)
        return pltpu.make_async_copy(obuf.at[slot], gate_out.at[rows], out_sem.at[0, slot])

    quarter = tiles // 4
    per_quarter = T // 4 // CHUNK

    def grad_at(q):
        rows = pl.ds(pl.multiple_of((q % per_quarter) * CHUNK, CHUNK), CHUNK)
        return q // (2 * per_quarter), (q // per_quarter) % 2, rows

    def grad_tile(t, slot):
        @pl.when(t >= 2)
        def _():
            put(t - 2, slot).wait()

        @pl.loop(0, TILE_ROWS // ROWS)
        def _(r):
            rows = pl.ds(r * ROWS, ROWS)
            at = pl.ds(t * TILE_ROWS + r * ROWS, ROWS)
            gv = zbuf[slot, rows, :].astype(F32)
            values = ybuf[slot, rows, :].astype(F32)
            sig = jax.nn.sigmoid(gv)
            silu = gv * sig
            gg = invc[at, 0:1] * nw_ref[...] * acc[at, :] - values * silu * cfc[at, 0:1]
            obuf[slot, rows, :] = (gg * values * sig * (1.0 + gv * (1.0 - sig))).astype(BF16)
            here = pl.ds((t % quarter) * TILE_ROWS + r * ROWS, ROWS)
            wbuf[t // (2 * quarter), (t // quarter) % 2, here, :] = (gg * silu).astype(BF16)

        put(t, slot).start()

    stream(grad_tile)
    for t in (tiles - 2, tiles - 1):
        put(t, t % 2).wait()

    pads = jnp.zeros((128 - HL, T), F32)
    cfc[...] = jnp.concatenate([ts_ref[...], pads], axis=0).T
    per = 2 * half // CHUNK

    def inside(q):
        plane = lax.rem(z + 1 + q // per, Z)
        r = q % per
        rows = half // CHUNK
        return plane, r // rows, pl.ds(pl.multiple_of((r % rows) * CHUNK, CHUNK), CHUNK)

    run[...] = jnp.zeros_like(run)

    @pl.loop(0, chunks, init_carry=jnp.zeros((1, 128), F32))
    def tail(step, later):
        q = chunks - 1 - step
        at = pl.ds(pl.multiple_of(q * CHUNK, CHUNK), CHUNK)
        total = last_of(q)
        sqp[at, :] = total - cum_col[at, :] + later
        grow = jnp.exp(cum_col[at, :])
        keep = jnp.exp(jnp.broadcast_to(total, (8, 128)))
        plane, hf, rows = inside(q)
        wa, wb, wr = grad_at(q)
        for g in range(NG):
            cols = slice(g * GW, (g + 1) * GW)
            scaled = (widen(grow, g) * wbuf[wa, wb, wr, cols].astype(F32)).astype(BF16)
            state = jnp.dot(c_ref[g, at, :].T, scaled, preferred_element_type=F32)
            pair[plane, hf, rows, cols] = run[:, cols].astype(BF16)
            run[:, cols] = state + widen(keep, g)[0:1, :] * run[:, cols]
        return later + total

    summ[c] = run[...].astype(BF16)
    keep_all = jnp.exp(jnp.broadcast_to(tail, (8, 128)))
    for g in range(NG):
        decay[c, :, g * GW : (g + 1) * GW] = widen(keep_all, g)

    def swaps():
        return (
            remote(summ.at[c], summ.at[c], swap_send.at[0], swap_recv.at[0], seq=partner),
            remote(decay.at[c], decay.at[c], swap_send.at[1], swap_recv.at[1], seq=partner),
        )

    for copy in swaps():
        copy.start()

    def state_left(part):
        rows = pl.ds(part * (NS // PARTS), NS // PARTS)
        return remote(
            vbuf.at[rows], rbuf.at[c, rows], st_send.at[part], st_recv.at[part], seq=s - 2
        )

    def state_swap(part):
        rows = pl.ds(part * (NS // PARTS), NS // PARTS)
        return remote(
            rbuf.at[c, rows], rbuf.at[c, rows], half_send.at[part], half_recv.at[part], seq=partner
        )

    mine_cols = pl.ds(pl.multiple_of(c * CH, CH), CH)

    def state_step(part):
        rows = pl.ds(part * (NS // PARTS), NS // PARTS)

        @pl.when(z < Z - 1)
        def _():
            state_left(part).wait_recv()
            state_swap(part).start()

        @pl.when(z > 0)
        def _():
            first_keep = decay[0, 0:1, mine_cols]
            here = summ[0, rows, mine_cols].astype(F32) + first_keep * summ[
                1, rows, mine_cols
            ].astype(F32)

            @pl.when(z < Z - 1)
            def _():
                vbuf[rows, :] = (
                    here
                    + first_keep * decay[1, 0:1, mine_cols] * rbuf[c, rows, :].astype(F32)
                ).astype(BF16)

            @pl.when(z == Z - 1)
            def _():
                vbuf[rows, :] = here.astype(BF16)

            state_left(part).start()

    upper = lax.broadcasted_iota(jnp.int32, (CHUNK, CHUNK), 1) >= lax.broadcasted_iota(
        jnp.int32, (CHUNK, CHUNK), 0
    )
    lane = lax.broadcasted_iota(jnp.int32, (CHUNK, 2 * HD), 1)

    @pl.loop(0, chunks)
    def _(q):
        @pl.when(q == 0)
        def _():
            for copy in swaps():
                copy.wait_recv()

        for part in range(PARTS):

            @pl.when(q == jnp.where(zm == 0, 0, jnp.minimum(2 * zm + part + 1, chunks - 1)))
            def _():
                state_step(part)

        at = pl.ds(pl.multiple_of(q * CHUNK, CHUNK), CHUNK)
        plane, hf, rows = inside(q)
        wa, wb, wr = grad_at(q)
        cum = cum_col[at, :]
        fade = jnp.exp(last_of(q) - cum)
        steps = cfc[at, :]
        skips = jnp.broadcast_to(skip_ref[...], (8, HL))
        for g in range(NG):
            b = b_ref[g, at, :]
            scores = lax.dot_general(
                b, c_ref[g, at, :], (((1,), (1,)), ((), ())), preferred_element_type=F32
            )
            scores = jnp.where(upper, scores, 0.0)
            cols = slice(g * GW, (g + 1) * GW)
            acc[at, cols] = widen(fade, g) * jnp.dot(
                b, pair[plane, hf, rows, cols], preferred_element_type=F32
            )
            for j in range(HPG // 2):
                weights = []
                for head in (g * HPG + 2 * j, g * HPG + 2 * j + 1):
                    gap = cum_row[head : head + 1, at] - cum[:, head : head + 1]
                    weights.append((scores * jnp.exp(jnp.minimum(gap, 0.0))).astype(BF16))
                span = slice(g * GW + 2 * j * HD, g * GW + 2 * (j + 1) * HD)
                both = wbuf[wa, wb, wr, span]
                zero = jnp.zeros_like(both)
                stacked = jnp.concatenate(
                    [jnp.where(lane < HD, both, zero), jnp.where(lane < HD, zero, both)], axis=0
                )
                acc[at, span] = acc[at, span] + jnp.dot(
                    jnp.concatenate(weights, axis=1), stacked, preferred_element_type=F32
                )
            acc[at, cols] = widen(steps, g) * acc[at, cols] + widen(skips, g)[0:1, :] * wbuf[
                wa, wb, wr, cols
            ].astype(F32)

    @pl.when(z > 0)
    def _():
        late_left(z - 1, half_of(z - 1, 1), 1).start()

    for ch in range(2):

        @pl.when(Z - 1 > z)
        def _():
            pair_copy(z, ch, 0, ch).wait_send()

        rs_prep(z, ch, 0, ch, ch)

    @pl.when(z < Z - 1)
    def _():
        for part in range(PARTS):
            rows = pl.ds(part * (NS // PARTS), NS // PARTS)
            remote(
                rbuf.at[1 - c, rows],
                rbuf.at[1 - c, rows],
                half_send.at[part],
                half_recv.at[part],
                seq=partner,
            ).wait_recv()

    @pl.when(z == Z - 1)
    def _():
        rbuf[...] = jnp.zeros_like(rbuf)

    for side in range(2):
        cols = slice(side * CH, (side + 1) * CH)
        later = rbuf[side].astype(F32)

        @pl.when(c == 1)
        def _():
            arrived[:, cols] = later.astype(BF16)

        @pl.when(c == 0)
        def _():
            arrived[:, cols] = (
                summ[1, :, cols].astype(F32) + decay[1, 0:1, cols] * later
            ).astype(BF16)

    def put_x(t, slot):
        rows = pl.ds(t * TILE_ROWS, TILE_ROWS)
        return pltpu.make_async_copy(ybuf.at[slot], gx_out.at[rows], out_sem.at[1, slot])

    @pl.loop(0, tiles)
    def _(t):
        slot = t % 2
        at = pl.ds(pl.multiple_of(t * TILE_ROWS, TILE_ROWS), TILE_ROWS)

        @pl.when(t >= 2)
        def _():
            put_x(t - 2, slot).wait()

        factor = cfc[at, :] * jnp.exp(sqp[at, :])
        for g in range(NG):
            cols = slice(g * GW, (g + 1) * GW)
            ybuf[slot, :, cols] = (
                acc[at, cols]
                + widen(factor, g)
                * jnp.dot(b_ref[g, at, :], arrived[:, cols], preferred_element_type=F32)
            ).astype(BF16)
        put_x(t, slot).start()

    scale = 1.0 / math.sqrt(T * S)

    def gow_copy(ch):
        rows = pl.ds(ch * half, half)
        return pltpu.make_async_copy(ownp.at[ch], gow_out.at[rows], out_sem.at[0, ch])

    for ch in range(2):
        pair_copy(z, ch, 0, ch).wait_recv()

        @pl.loop(0, half // ROWS)
        def _(r):
            at = pl.ds(r * ROWS, ROWS)
            ownp[ch, at, :] = ownp[ch, at, :] + pair[z, ch, at, :].astype(F32)

    for first, from_slot in ((0, z), (Z - 1, Z)):
        for step in range(2):

            @pl.when(z != first)
            def _():
                ch = half_of(z, step)
                if first == Z - 1 and step == 1:
                    late_arrived(ch, 0)
                    late_arrived(ch, 1)
                else:
                    chain_arrived(from_slot, ch)

                @pl.loop(0, half // ROWS)
                def _(r):
                    at = pl.ds(r * ROWS, ROWS)
                    ownp[ch, at, :] = ownp[ch, at, :] + chain[from_slot, ch, at, :].astype(F32)

    for ch in range(2):

        @pl.loop(0, half // ROWS)
        def _(r):
            at = pl.ds(r * ROWS, ROWS)
            ownp[ch, at, :] = ownp[ch, at, :] * scale

        gow_copy(ch).start()

    for t in (tiles - 2, tiles - 1):
        put_x(t, t % 2).wait()

    for copy in swaps():
        copy.wait_send()
    for part in range(PARTS):

        @pl.when(z < Z - 1)
        def _():
            state_swap(part).wait_send()

        @pl.when(z > 0)
        def _():
            state_left(part).wait_send()

    for ch in range(2):
        pair_copy(z, ch, 0, ch).wait_send()

        @pl.when(z > 0)
        def _():
            pair_copy(z, ch, 1, ch).wait_send()

        @pl.loop(0, Z)
        def _(k):
            w_swap(k, ch).wait_send()

            @pl.when(jnp.logical_and(k <= z, z < Z - 1))
            def _():
                w_right(k, ch).wait_send()

            @pl.when(jnp.logical_and(k >= z, z > 0))
            def _():
                w_left(k, ch).wait_send()

            @pl.when(k > z)
            def _():
                chain_right(k, ch).wait_send()

            late = jnp.logical_and(k == z - 1, half_of(k, 1) == ch)

            @pl.when(jnp.logical_and(k < z, late))
            def _():
                late_left(k, ch, 0).wait_send()
                late_left(k, ch, 1).wait_send()

            @pl.when(jnp.logical_and(k < z, jnp.logical_not(late)))
            def _():
                chain_left(k, ch).wait_send()

    for sub in subs:
        if H == 4:
            g_relay(2, 1, sub, 0).wait_send()
            g_relay(1, 2, sub, 1).wait_send()
        for j in others if H != 4 else (1, 2):
            for hf in range(2):
                g_to(j, sub, hf).wait_send()
    for ch in range(2):
        gow_copy(ch).wait()


def mixer(
    grad_output,
    out_weight,
    ssd_out,
    gate,
    norm_weight,
    time_step,
    log_decay,
    state_in,
    state_out,
    skip,
):
    S, H = lax.axis_size("seq"), lax.axis_size("head")
    T, F = grad_output.shape
    Wr, C = out_weight.shape
    Z = S // 2
    half = Wr // 2
    nsub = F // Wr
    heads_here = time_step.shape[0]
    groups_here = max(1, heads_here * GROUPS // HEADS)
    NS = state_in.shape[2]
    hbm = pl.BlockSpec(memory_space=pl.ANY)
    vmem = pl.BlockSpec(memory_space=pltpu.VMEM)
    dma = pltpu.SemaphoreType.DMA
    flops = 4 * T * F * H * C
    outs = pl.pallas_call(
        functools.partial(mixer_kernel, (S, H, T, F, Wr, C)),
        out_shape=(
            jax.ShapeDtypeStruct((T, C), BF16),
            jax.ShapeDtypeStruct((T, C), BF16),
            jax.ShapeDtypeStruct((Wr, C), F32),
            jax.ShapeDtypeStruct((S, 2, half, C), BF16),
        ),
        in_specs=[hbm] * 4 + [vmem] * 3 + [hbm] * 2 + [vmem],
        out_specs=(hbm,) * 4,
        scratch_shapes=[
            pltpu.VMEM((S, 2, T, half), BF16),
            pltpu.VMEM((T, C), BF16),
            pltpu.VMEM((T, C), F32),
            pltpu.VMEM((Z, 2, half, C), BF16),
            pltpu.VMEM((Z + 1, 2, half, C), BF16),
            pltpu.VMEM((2, 2, half, C), BF16),
            pltpu.VMEM((2, half, C), F32),
            pltpu.VMEM((Wr, T), BF16),
            pltpu.VMEM((2, 2, max(half, T // 4), C), BF16),
            pltpu.VMEM((2, TILE_ROWS, C), BF16),
            pltpu.VMEM((2, TILE_ROWS, C), BF16),
            pltpu.VMEM((2, TILE_ROWS, C), BF16),
            pltpu.VMEM((T, 128), F32),
            pltpu.VMEM((H, 8, T), F32),
            pltpu.VMEM((H, 8, T), F32),
            pltpu.VMEM((T, 128), F32),
            pltpu.VMEM((T, 128), F32),
            pltpu.VMEM((128, T), F32),
            pltpu.VMEM((T, 128), F32),
            pltpu.VMEM((128, C), BF16),
            pltpu.VMEM((NS, C), F32),
            pltpu.VMEM((2, NS, C), BF16),
            pltpu.VMEM((2, 8, C), F32),
            pltpu.VMEM((2, NS, C // 2), BF16),
            pltpu.VMEM((NS, C // 2), BF16),
            pltpu.VMEM((NS, C), BF16),
            pltpu.VMEM((2, CHUNK, GROUPS, NS), BF16),
            pltpu.VMEM((groups_here, T, NS), BF16),
            pltpu.VMEM((groups_here, T, NS), BF16),
            dma((S, 2)),
            dma((Z, 2)),
            dma((Z, 2)),
            dma((Z, 2)),
            dma((S, 2)),
            dma((H, nsub, 2)),
            dma((H,)),
            dma((H,)),
            dma((H,)),
            dma((H,)),
            dma((Z, 2)),
            dma((2, 2)),
            dma((Z + 1, 2)),
            dma((Z, 2)),
            dma((nsub, 2)),
            dma((2, 2)),
            dma((2, 2)),
            dma((2, 2)),
            dma((2,)),
            dma((2,)),
            dma((4,)),
            dma((4,)),
            dma((4,)),
            dma((4,)),
            dma((2,)),
        ],
        compiler_params=pltpu.CompilerParams(
            collective_id=0, has_side_effects=True, vmem_limit_bytes=67043328
        ),
        cost_estimate=pl.CostEstimate(flops=flops, bytes_accessed=64 << 20, transcendentals=0),
        name="mixer",
    )(
        grad_output,
        out_weight,
        ssd_out,
        gate,
        norm_weight.reshape(1, C),
        time_step,
        log_decay,
        state_in,
        state_out,
        skip.reshape(1, heads_here),
    )
    grad_gate, grad_x, grad_out_weight, _ = outs
    return grad_x, grad_gate, grad_out_weight


def solution(mesh):
    return jax.shard_map(
        mixer,
        mesh=mesh,
        in_specs=(
            P("seq", "head"),
            P("seq", "head"),
            P("seq", "head"),
            P("seq", "head"),
            P("head"),
            P("head", "seq"),
            P("head", "seq"),
            P("seq", None, None),
            P("seq", None, None),
            P("head"),
        ),
        out_specs=(P("seq", "head"), P("seq", "head"), P("seq", "head")),
        check_vma=False,
    )
```
